128 devices in a mesh: lat: 8 (over x_hi, y), lon: 16 (over x_lo, z, core).
Axes of the slice: x: 4 (x_hi: 2, x_lo: 2; x = x_hi * 2 + x_lo), y: 4, z: 4, core: 2. Of those that a mesh axis runs over, the one named last changes fastest.
Arguments:
- right_side: float32 [1024, 4096], P('lat', 'lon'), may hold values from -12 to 12
- diagonal: float32 [1024, 4096], P('lat', 'lon'), may hold values from 0.2 to 2
- east_coef: float32 [1024, 4096], P('lat', 'lon'), may hold values from 0.5 to 2
- north_coef: float32 [1024, 4096], P('lat', 'lon'), may hold values from 0.5 to 2
- land_sea: int32 [1024, 4096], P('lat', 'lon'), may hold values 0 or 1
- fold_partner: int32 [4096], P('lon'), may hold values from 0 to 4095, as said below
Outputs:
- solution_field: float32 [1024, 4096], P('lat', 'lon')
- residual: float32 [1024, 4096], P('lat', 'lon')
The draws below stay inside these ranges and needn't reach their ends.
Inputs may be any that keep to these rules, and one draw needn't show every extreme that they name: fold_partner[fold_partner[i]] = i and fold_partner[i] != i for every column i, and fold_partner[i] // 256 = 15 - i // 256.
All inputs are finite; a program needn't handle non-finite values. No bound on the sum of `land_sea` on one device may be relied on, other than what follows from the above.
Results may differ from the reference program's by a relative error of at most 0.00019.
Values sent between devices are 32-bit elements; how exact they have to be, the bound alone decides.
No kernel may reach another device: no remote copies, remote signals or barrier semaphores. Data moves between devices by JAX's collectives and lax.ppermute only.
A program may use at most 64 MiB of HBM per device.

```python
import math
import jax
import jax.numpy as jnp

CI = 256
ITERS = 4
NJ = 1024
NI = 4096


def draw_right_side(key, part):
    first_key, second_key, third_key = jax.random.split(key, 3)
    row_pos = jnp.arange(NJ, dtype=jnp.float32) / NJ
    col_pos = jnp.arange(NI, dtype=jnp.float32) / NI
    row_scale = jnp.exp(0.6 * row_pos - 0.6 + jax.random.uniform(first_key, (NJ,), jnp.float32, -0.6, 0.6))
    col_scale = jnp.exp(0.6 * col_pos - 0.6 + jax.random.uniform(second_key, (NI,), jnp.float32, -0.6, 0.6))
    scaled = row_scale[:, None] * col_scale[None, :]
    values = jax.random.normal(third_key, (NJ, NI), jnp.float32) * scaled
    return jnp.clip(values, -12.0, 12.0)


def draw_fold_partner(key, part):
    block_count = NI // CI
    pair_count = block_count // 2
    pair_keys = jax.random.split(key, pair_count)

    def mirror_order(subkey):
        return jax.random.permutation(subkey, CI)
    shuffled = jax.vmap(mirror_order)(pair_keys).astype(jnp.int32)
    pair_ids = jnp.arange(pair_count, dtype=jnp.int32)
    lower_cols = (pair_ids[:, None] * CI + jnp.arange(CI, dtype=jnp.int32)[None, :]).reshape(-1)
    upper_cols = ((block_count - 1 - pair_ids)[:, None] * CI + shuffled).reshape(-1)
    partner = jnp.zeros((NI,), jnp.int32).at[lower_cols].set(upper_cols)
    return partner.at[upper_cols].set(lower_cols)


def plant(array, own_key, least, top_value):
    longest = array.shape.index(max(array.shape))
    spots = []
    for shift in (0, 1):
        where = [jax.random.randint(jax.random.fold_in(own_key, axis), (), 0, length) for axis, length in enumerate(array.shape)]
        where[longest] = (where[longest] + shift) % array.shape[longest]
        spots.append(tuple(where))
    return array.at[spots[0]].set(least).at[spots[1]].set(top_value)


def levels(key, shape, cuts, least, largest):
    loudness, own = 1.0, jax.random.fold_in(key, 6)
    for axis_at, parts in cuts:
        heights = jnp.exp(jax.random.uniform(jax.random.fold_in(own, axis_at), (parts,), jnp.float32, least / len(cuts), largest / len(cuts)))
        loudness = loudness * jnp.repeat(heights, shape[axis_at] // parts).reshape([-1 if axis == axis_at else 1 for axis in range(len(shape))])
    return loudness


def setup_inputs(seed: int = 0) -> dict:
    key_of = jax.random.split(jax.random.key(seed), 7)
    right_side = draw_right_side(jax.random.fold_in(key_of[6], 71), 0)
    diagonal = jnp.clip(jnp.exp(math.log(2.0) - 2.3025851 * jax.random.uniform(key_of[1], (NJ, NI), jnp.float32) ** levels(key_of[1], (NJ, NI), ((0, 8), (1, 16)), -0.2, 0.2)), 0.2, 2.0)
    east_coef = jnp.clip(jnp.exp(math.log(2.0) - 1.3862944 * jax.random.uniform(key_of[2], (NJ, NI), jnp.float32) ** levels(key_of[2], (NJ, NI), ((0, 8), (1, 16)), -0.2, 0.2)), 0.5, 2.0)
    north_coef = jnp.clip(jnp.exp(math.log(2.0) - 1.3862944 * jax.random.uniform(key_of[3], (NJ, NI), jnp.float32) ** levels(key_of[3], (NJ, NI), ((0, 8), (1, 16)), -0.2, 0.2)), 0.5, 2.0)
    land_sea = plant((jax.random.randint(key_of[4], (NJ, NI), 0, 10) < 7).astype(jnp.int32), jax.random.fold_in(key_of[4], 1), 0, 1)
    fold_partner = draw_fold_partner(jax.random.fold_in(key_of[6], 71), 0)
    return {"right_side": right_side, "diagonal": diagonal, "east_coef": east_coef, "north_coef": north_coef, "land_sea": land_sea, "fold_partner": fold_partner}


def spread_of(masked, east_coef, north_coef, fold_partner):
    west_coef = jnp.roll(east_coef, 1, axis=1)
    north_inner = north_coef.at[-1].set(0.0)
    blank = jnp.zeros_like(masked[:1])
    north_vals = jnp.concatenate([masked[1:], blank], axis=0)
    south_vals = jnp.concatenate([blank, masked[:-1]], axis=0)
    south_coef = jnp.concatenate([jnp.zeros_like(north_inner[:1]), north_inner[:-1]], axis=0)
    top_coef = north_coef[-1]
    fold_coef = 0.5 * (top_coef + top_coef[fold_partner])
    spread = east_coef * (masked - jnp.roll(masked, -1, axis=1)) + west_coef * (masked - jnp.roll(masked, 1, axis=1))
    spread = spread + north_inner * (masked - north_vals) + south_coef * (masked - south_vals)
    last_row = masked[-1]
    return spread.at[-1].add(fold_coef * (last_row - last_row[fold_partner]))


def reference(right_side, diagonal, east_coef, north_coef, land_sea, fold_partner):
    ocean = land_sea.astype(jnp.float32)

    def operate(surface):
        masked = ocean * surface
        return diagonal * surface + ocean * spread_of(masked, east_coef, north_coef, fold_partner)

    solution_field = jnp.zeros_like(right_side)
    residual = right_side
    direction = right_side
    norm_now = jnp.sum(residual * residual)
    for iteration in range(ITERS):
        image = operate(direction)
        alpha = norm_now / jnp.sum(direction * image)
        solution_field = solution_field + alpha * direction
        residual = residual - alpha * image
        norm_next = jnp.sum(residual * residual)
        direction = residual + (norm_next / norm_now) * direction
        norm_now = norm_next
    return solution_field, residual
```

```python
import functools

import jax
import jax.numpy as jnp
from jax import lax
from jax.experimental import pallas as pl
from jax.experimental.pallas import tpu as pltpu
from jax.sharding import Mesh
from jax.sharding import PartitionSpec as P

ITERS = 4
LAT_LON = ("lat_0", "lat_1", "lon_0", "lon_1", "lon_2")
LAT = ("lat_0", "lat_1")
LON = ("lon_0", "lon_1", "lon_2")
MID = 4.6
HALF = 4.4
F32 = jnp.float32
W = 4
LANES = 128
STRIP = 48


def _iota(shape, axis):
    return lax.broadcasted_iota(jnp.int32, shape, axis)


def _cat(parts, axis):
    return jnp.concatenate(parts, axis=axis)


def _pack_rows(*refs):
    bottoms, tops, (partner, south_out, north_out) = (refs[:5], refs[5:10], refs[10:])
    south_out[...] = jnp.zeros_like(south_out)
    north_out[...] = jnp.zeros_like(north_out)
    for f in range(5):
        south_out[W * f : W * f + W, :] = bottoms[f][0:W, :].astype(F32)
        north_out[W * f : W * f + W, :] = tops[f][8 - W : 8, :].astype(F32)
    north_out[20:21, :] = partner[...].astype(F32)


def pack_rows(fields, partner):
    rows, cols = fields[0].shape
    low = pl.BlockSpec((8, cols), lambda i: (0, 0))
    high = pl.BlockSpec((8, cols), lambda i: (rows // 8 - 1, 0))
    out = jax.ShapeDtypeStruct((24, cols), F32)
    return pl.pallas_call(
        _pack_rows,
        grid=(1,),
        in_specs=[low] * 5 + [high] * 5 + [pl.BlockSpec((1, cols), lambda i: (0, 0))],
        out_specs=(pl.BlockSpec((24, cols), lambda i: (0, 0)),) * 2,
        out_shape=(out, out),
        name="pack_rows",
    )(*fields, *fields, partner)


def _pick(source, index):
    low = index & (LANES - 1)
    outs = []
    for t in range(2):
        at = low[:, t * LANES : (t + 1) * LANES]
        first = jnp.take_along_axis(source[:, :LANES], at, axis=1)
        second = jnp.take_along_axis(source[:, LANES:], at, axis=1)
        outs.append(jnp.where(index[:, t * LANES : (t + 1) * LANES] < LANES, first, second))
    return _cat(outs, 1)


def _pack_cols(top, r, oc, dg, ea, no, from_n, from_s, from_m, own_top, to_w, to_e, strip):
    rows = r.shape[0]
    lane = _iota((1, LANES), 1)

    def packed(pieces):
        west = east = None
        for f, (left, right) in enumerate(pieces):
            a = left if f == 0 else pltpu.roll(left, W * f, 1)
            b = pltpu.roll(right, W * f + W, 1)
            if f == 0:
                west, east = (a, b)
            else:
                here = lane >= W * f
                west = jnp.where(here, a, west)
                east = jnp.where(here, b, east)
        used = lane < 5 * W
        return (jnp.where(used, west, 0.0), jnp.where(used, east, 0.0))

    zero = jnp.zeros((W, LANES), F32)
    for start in range(0, rows, 32):
        span = pl.ds(start, 32)
        west, east = packed(
            [(x[span, :LANES].astype(F32), x[span, LANES:].astype(F32)) for x in (r, oc, dg, ea, no)]
        )
        to_w[pl.ds(8 + start, 32), :] = west
        to_e[pl.ds(8 + start, 32), :] = east
    for src, base, blank in ((from_s, 4, 0), (from_n, 8 + rows, 12 + rows)):
        west, east = packed(
            [(src[W * f : W * f + W, :LANES], src[W * f : W * f + W, LANES:]) for f in range(5)]
        )
        to_w[base : base + W, :] = west
        to_e[base : base + W, :] = east
        to_w[blank : blank + W, :] = zero
        to_e[blank : blank + W, :] = zero

    @pl.when(top[0] == 1)
    def _():
        for f in range(5):
            strip[8 * f : 8 * f + W, :] = own_top[W * f : W * f + W, :]
            strip[8 * f + W : 8 * f + 8, :] = from_m[W * f : W * f + W, :]
        strip[40:48, :] = jnp.zeros((8, 2 * LANES), F32)
        own_partner, far_partner = (own_top[20:21, :], from_m[20:21, :])
        strip[40:41, :] = own_partner
        strip[41:42, :] = far_partner
        row = _iota((8, 1), 0)
        index = jnp.where(row < 4, own_partner, far_partner).astype(jnp.int32) & (2 * LANES - 1)
        masked = strip[0:8, :] * strip[8:16, :]
        first = _pick(pltpu.roll(masked, 4, 0), index)
        north = strip[32:40, :]
        coef = 0.5 * (north + _pick(pltpu.roll(north, 4, 0), index))
        strip[35:36, :] = coef[3:4, :]
        strip[39:40, :] = coef[7:8, :]
        strip[42:43, :] = first[3:4, :]
        strip[43:44, :] = first[7:8, :]

    base = rows + 16
    for half in range(2):
        part = strip[:, half * LANES : (half + 1) * LANES]
        to_w[base + STRIP * half : base + STRIP * (half + 1), :] = part
        to_e[base + STRIP * half : base + STRIP * (half + 1), :] = part


def pack_cols(top, fields, from_n, from_s, from_m, own_top):
    rows, cols = fields[0].shape
    message = jax.ShapeDtypeStruct((rows + 16 + 2 * STRIP, LANES), F32)
    vmem = pl.BlockSpec(memory_space=pltpu.VMEM)
    return pl.pallas_call(
        _pack_cols,
        in_specs=[pl.BlockSpec(memory_space=pltpu.SMEM)] + [vmem] * 9,
        out_specs=(vmem,) * 3,
        out_shape=(message, message, jax.ShapeDtypeStruct((STRIP, cols), F32)),
        name="pack_cols",
    )(top, *fields, from_n, from_s, from_m, own_top)


def _lanes_left(x):
    return pltpu.roll(x, x.shape[1] - 1, 1)


def _lanes_right(x):
    return pltpu.roll(x, 1, 1)


def _strip_levels(strip, from_e, from_w, e2, w2, fold, base):
    row = _iota((8, 1), 0)
    lane = _iota((1, LANES), 1)
    near = row < 4

    def far(ref, at, count):
        return _cat(
            [ref[base + at : base + at + count, :], ref[base + STRIP + at : base + STRIP + at + count, :]], 1
        )

    def assembled(mine, east, west, east2, west2):
        left = jnp.where(near, west, east)
        right = jnp.where(near, east, west)
        tail = jnp.where(
            lane < 64,
            jnp.where(near, east2, west2)[:, :LANES],
            jnp.where(near, west2, east2)[:, LANES:],
        )
        return _cat([left, mine, right, tail], 1)

    def field(f):
        s = 8 * f
        return assembled(
            strip[s : s + 8, :], far(from_e, s, 8), far(from_w, s, 8), e2[s : s + 8, :], w2[s : s + 8, :]
        )

    def pair(at):
        def one(a, b):
            return jnp.where(near, a, b)

        return assembled(
            one(strip[at : at + 1, :], strip[at + 1 : at + 2, :]),
            one(far(from_e, at, 1), far(from_e, at + 1, 1)),
            one(far(from_w, at, 1), far(from_w, at + 1, 1)),
            one(e2[at : at + 1, :], e2[at + 1 : at + 2, :]),
            one(w2[at : at + 1, :], w2[at + 1 : at + 2, :]),
        )

    r, oc, dg, ea, no = [field(f) for f in range(5)]
    index = pair(40).astype(jnp.int32) & (2 * LANES - 1)
    neighbour = pair(42)
    edge = (row & 3) == 3
    fc = jnp.where(edge, no, 0.0)
    no = jnp.where(edge, 0.0, no)
    scale = 2.0 / HALF
    ocs = oc * scale
    ce = ea * ocs * _lanes_left(oc)
    cw = _lanes_right(ce)
    cn = no * ocs * pltpu.roll(oc, 7, 0)
    cs = pltpu.roll(cn, 1, 0)
    cf = fc * ocs
    d = (dg - MID) * scale + ocs * (ea + _lanes_right(ea) + no + pltpu.roll(no, 1, 0) + fc)

    def main_row(x):
        x = x[3:4, :]
        return _cat([x[:, 256:512], jnp.where(lane < 64, x[:, 512:640], x[:, 128:256])], 1)

    fold[4:5, :] = main_row(cf)
    previous = None
    value = r
    for k in range(4):
        term = cf * neighbour
        fold[k : k + 1, :] = main_row(term)
        if k == 3:
            break
        new = (
            d * value
            - ce * _lanes_left(value)
            - cw * _lanes_right(value)
            - cn * pltpu.roll(value, 7, 0)
            - cs * pltpu.roll(value, 1, 0)
            - term
        )
        new = 0.5 * new if k == 0 else new - previous
        previous, value = (value, new)
        swapped = pltpu.roll(value * oc, 4, 0)
        blocks = [swapped[:, 256 * j : 256 * j + 256] for j in range(3)]
        picked = [_pick(blocks[2 - j], index[:, 256 * j : 256 * j + 256]) for j in range(3)]
        neighbour = _cat([*picked, jnp.zeros((8, LANES), F32)], 1)


def _basis(top, r, oc, dg, ea, no, from_n, from_s, from_e, from_w, strip, e2, w2, t1, t2, t3, t4, moments, ext, coef, fold):
    rows, cols = r.shape
    pad = 16
    high = rows + pad
    wide = cols + LANES
    lane = _iota((1, LANES), 1)
    total = rows + 2 * pad
    on_top = top[0] == 1
    for f, own in enumerate((r, oc, dg, ea, no)):
        ext[f, 0 : pad, :cols] = jnp.zeros((pad, cols), F32)
        ext[f, high : high + pad, :cols] = jnp.zeros((pad, cols), F32)
        ext[f, pad:high, :cols] = own[...].astype(F32)
        ext[f, pad - W : pad, :cols] = from_s[W * f : W * f + W, :]
        ext[f, high : high + W, :cols] = from_n[W * f : W * f + W, :]
        ext[f, 0:8, cols:] = jnp.zeros((8, LANES), F32)
        ext[f, total - 8 : total, cols:] = jnp.zeros((8, LANES), F32)
        east = from_e[0 : rows + 16, :]
        if f:
            east = pltpu.roll(east, LANES - W * f, 1)
        west = pltpu.roll(from_w[0 : rows + 16, :], LANES - W - W * f, 1)
        halo = jnp.where(lane < W, east, jnp.where(lane >= LANES - W, west, 0.0))
        ext[f, 8 : 8 + rows + 16, cols:] = halo
    for k in (5, 6, 7):
        ext[k, 0:8, :] = jnp.zeros((8, wide), F32)
        ext[k, total - 8 : total, :] = jnp.zeros((8, wide), F32)

    @pl.when(on_top)
    def _():
        ext[4, high - 1 : high, :] = jnp.zeros((1, wide), F32)
        _strip_levels(strip, from_e, from_w, e2, w2, fold, rows + 16)

    @pl.when(jnp.logical_not(on_top))
    def _():
        fold[...] = jnp.zeros_like(fold)

    scale = 2.0 / HALF
    last = (high - 8) // 8
    sub = _iota((8, 1), 0)
    for t in range(1, total // 8 - 1):
        a = 8 * t
        o = ext[1, a : a + 8, :]
        os = o * scale
        e = ext[3, a : a + 8, :]
        n = ext[4, a : a + 8, :]
        d = (ext[2, a : a + 8, :] - MID) * scale + os * (e + _lanes_right(e) + n + ext[4, a - 1 : a + 7, :])
        if t == last:
            d = d + jnp.where(sub == 7, fold[4:5, :], 0.0)
        coef[0, a : a + 8, :] = d
        coef[1, a : a + 8, :] = e * os * _lanes_left(o)
        coef[2, a : a + 8, :] = n * os * ext[1, a + 1 : a + 9, :]
    coef[2, 0:8, :] = jnp.zeros((8, wide), F32)

    outs = (t1, t2, t3, t4)
    sums = []
    own = r[0:8, :]
    square = own * own
    for t in range(1, rows // 8):
        own = r[8 * t : 8 * t + 8, :]
        square = square + own * own
    sums.append(square)
    for k in range(4):
        source = 0 if k == 0 else 4 + k
        square = cross = None
        tiles = range(2, total // 8 - 2) if k == 3 else range(1, total // 8 - 1)
        for t in tiles:
            a = 8 * t
            v = ext[source, a : a + 8, :]
            ce = coef[1, a : a + 8, :]
            new = (
                coef[0, a : a + 8, :] * v
                - ce * _lanes_left(v)
                - _lanes_right(ce * 1.0) * _lanes_right(v)
                - coef[2, a : a + 8, :] * ext[source, a + 1 : a + 9, :]
                - coef[2, a - 1 : a + 7, :] * ext[source, a - 1 : a + 7, :]
            )
            if t == last:
                new = new - jnp.where(sub == 7, fold[k : k + 1, :], 0.0)
            if k == 0:
                new = 0.5 * new
            else:
                new = new - ext[0 if k == 1 else 3 + k, a : a + 8, :]
            if k < 3:
                ext[5 + k, a : a + 8, :] = new
            if pad <= a < high:
                mine = new[:, :cols]
                outs[k][a - pad : a - pad + 8, :] = mine
                x = mine * v[:, :cols]
                cross = x if cross is None else cross + x
                if k < 3:
                    s = mine * mine
                    square = s if square is None else square + s
        sums.append(cross)
        if k < 3:
            sums.append(square)
    out = jnp.zeros((1, LANES), F32)
    for k, x in enumerate(sums):
        folded = x[:, :LANES] + x[:, LANES:]
        one = jnp.sum(jnp.sum(folded, axis=0, keepdims=True), axis=1, keepdims=True)
        out = jnp.where(lane == k, one, out)
    moments[...] = jnp.broadcast_to(out, moments.shape)


def basis(top, fields, from_n, from_s, from_e, from_w, strip, e2, w2, devices):
    rows, cols = fields[0].shape
    vmem = pl.BlockSpec(memory_space=pltpu.VMEM)
    out = jax.ShapeDtypeStruct((rows, cols), F32)
    return pl.pallas_call(
        _basis,
        in_specs=[pl.BlockSpec(memory_space=pltpu.SMEM)] + [vmem] * 12,
        out_specs=(vmem,) * 5,
        out_shape=(out,) * 4 + (jax.ShapeDtypeStruct((devices, LANES), F32),),
        scratch_shapes=[
            pltpu.VMEM((8, rows + 32, cols + LANES), F32),
            pltpu.VMEM((3, rows + 32, cols + LANES), F32),
            pltpu.VMEM((8, cols + LANES), F32),
        ],
        name="basis",
    )(top, *fields, from_n, from_s, from_e, from_w, strip, e2, w2)


def _combine(gathered, r, t1, t2, t3, t4, x_out, r_out):
    sums = jnp.sum(gathered[...], axis=0, keepdims=True)
    m = [sums[:, k : k + 1] for k in range(8)]
    nu = [m[0], m[1]]
    for k in range(1, 4):
        nu += [2.0 * m[2 * k] - m[0], 2.0 * m[2 * k + 1] - m[1]]
    gram = {}
    for i in range(4):
        for j in range(i, 5):
            if i == 0:
                gram[i, j] = nu[j]
            else:
                gram[i, j] = 0.5 * (nu[i + j] + nu[j - i])
            gram[j, i] = gram[i, j]

    def dot(a, b):
        total = None
        for i, p in enumerate(a):
            inner = None
            for j, q in enumerate(b):
                term = q * gram[i, j]
                inner = term if inner is None else inner + term
            inner = p * inner
            total = inner if total is None else total + inner
        return total

    def apply(v):
        n = len(v)
        out = [MID * x for x in v] + [None]
        for j, x in enumerate(v):
            if j == 0:
                up = HALF * x
            else:
                up = (0.5 * HALF) * x
                out[j - 1] = out[j - 1] + up
            out[j + 1] = up if out[j + 1] is None else out[j + 1] + up
        return out

    def add(a, s, b):
        out = []
        for i in range(max(len(a), len(b))):
            if i >= len(a):
                out.append(s * b[i])
            elif i >= len(b):
                out.append(a[i])
            else:
                out.append(a[i] + s * b[i])
        return out

    one = jnp.ones((1, 1), F32)
    solution_field, residual, direction = ([], [one], [one])
    norm_now = m[0]
    for iteration in range(ITERS):
        image = apply(direction)
        alpha = norm_now / dot(direction, image)
        solution_field = add(solution_field, alpha, direction)
        residual = add(residual, -alpha, image)
        if iteration + 1 < ITERS:
            norm_next = dot(residual, residual)
            direction = add(residual, norm_next / norm_now, direction)
            norm_now = norm_next
    basis_refs = (r, t1, t2, t3, t4)
    for start in range(0, r.shape[0], 8):
        span = pl.ds(start, 8)
        tiles = [ref[span, :] for ref in basis_refs]
        x = solution_field[0] * tiles[0]
        z = residual[0] * tiles[0]
        for k in range(1, 5):
            if k < 4:
                x = x + solution_field[k] * tiles[k]
            z = z + residual[k] * tiles[k]
        x_out[span, :] = x
        r_out[span, :] = z


def combine(gathered, r, t1, t2, t3, t4):
    vmem = pl.BlockSpec(memory_space=pltpu.VMEM)
    out = jax.ShapeDtypeStruct(r.shape, F32)
    return pl.pallas_call(
        _combine, in_specs=[vmem] * 6, out_specs=(vmem,) * 2, out_shape=(out, out), name="combine"
    )(gathered, r, t1, t2, t3, t4)


def local(right_side, diagonal, east_coef, north_coef, land_sea, fold_partner):
    cols = right_side.shape[1]
    lats, lons = (lax.axis_size(LAT), lax.axis_size(LON))
    devices = lats * lons
    top = (lax.axis_index(LAT) == lats - 1).astype(jnp.int32).reshape(1)
    fields = (right_side, land_sea, diagonal, east_coef, north_coef)

    def at(i, j):
        return i * lons + j % lons

    def top_row(x, partner):
        return lax.ppermute(x, LAT_LON, [(at(lats - 1, partner(j)), at(lats - 1, j)) for j in range(lons)])

    to_south, to_north = pack_rows(fields, fold_partner.reshape(1, cols))
    from_m = top_row(to_north, lambda j: lons - 1 - j)
    from_n = lax.ppermute(to_south, LAT, [(i + 1, i) for i in range(lats - 1)])
    from_s = lax.ppermute(to_north, LAT, [(i, i + 1) for i in range(lats - 1)])
    to_w, to_e, strip = pack_cols(top, fields, from_n, from_s, from_m, to_north)
    e2 = top_row(strip, lambda j: j + 2)
    w2 = top_row(strip, lambda j: j - 2)
    from_e = lax.ppermute(to_w, LON, [((j + 1) % lons, j) for j in range(lons)])
    from_w = lax.ppermute(to_e, LON, [(j, (j + 1) % lons) for j in range(lons)])
    t1, t2, t3, t4, moments = basis(
        top, fields, from_n, from_s, from_e, from_w, strip, e2, w2, devices
    )
    gathered = lax.all_to_all(moments, LAT_LON, 0, 0)
    return combine(gathered, right_side, t1, t2, t3, t4)


def solution(mesh):
    torus = Mesh(mesh.devices.reshape(2, 4, 2, 4, 2), ("lat_0", "lat_1", "lon_0", "lon_1", "lon_2"))
    placed = (P(LAT, LON), P(LAT, LON), P(LAT, LON), P(LAT, LON), P(LAT, LON), P(LON))
    return jax.shard_map(
        local, mesh=torus, in_specs=placed, out_specs=(P(LAT, LON), P(LAT, LON)), check_vma=False
    )
```

```python
import functools

import jax
import jax.numpy as jnp
from jax import lax
from jax.experimental import pallas as pl
from jax.experimental.pallas import tpu as pltpu
from jax.sharding import Mesh
from jax.sharding import PartitionSpec as P

ITERS = 4
LAT_LON = ("lat_0", "lat_1", "lon_0", "lon_1", "lon_2")
LAT = ("lat_0", "lat_1")
LON = ("lon_0", "lon_1", "lon_2")
MID = 4.6
HALF = 4.4
F32 = jnp.float32
W = 4
LANES = 128
STRIP = 48


def _iota(shape, axis):
    return lax.broadcasted_iota(jnp.int32, shape, axis)


def _cat(parts, axis):
    return jnp.concatenate(parts, axis=axis)


def _pack_rows(flags, *refs):
    bottoms, tops, (partner, first, second) = (refs[:5], refs[5:10], refs[10:])
    even = flags[1] == 0
    for f in range(5):
        low = bottoms[f][0:W, :].astype(F32)
        high = tops[f][8 - W : 8, :].astype(F32)
        first[W * f : W * f + W, :] = jnp.where(even, high, low)
        second[W * f : W * f + W, :] = jnp.where(even, low, high)
    first[20:24, :] = jnp.zeros((4, first.shape[1]), F32)
    second[20:24, :] = jnp.broadcast_to(partner[...].astype(F32), (4, first.shape[1]))


def pack_rows(flags, fields, partner):
    rows, cols = fields[0].shape
    low = pl.BlockSpec((8, cols), lambda i: (0, 0))
    high = pl.BlockSpec((8, cols), lambda i: (rows // 8 - 1, 0))
    out = jax.ShapeDtypeStruct((24, cols), F32)
    return pl.pallas_call(
        _pack_rows,
        grid=(1,),
        in_specs=[pl.BlockSpec(memory_space=pltpu.SMEM)]
        + [low] * 5
        + [high] * 5
        + [pl.BlockSpec((1, cols), lambda i: (0, 0))],
        out_specs=(pl.BlockSpec((24, cols), lambda i: (0, 0)),) * 2,
        out_shape=(out, out),
        name="pack_rows",
    )(flags, *fields, *fields, partner)


def _pick(source, index):
    low = index & (LANES - 1)
    outs = []
    for t in range(2):
        at = low[:, t * LANES : (t + 1) * LANES]
        first = jnp.take_along_axis(source[:, :LANES], at, axis=1)
        second = jnp.take_along_axis(source[:, LANES:], at, axis=1)
        outs.append(jnp.where(index[:, t * LANES : (t + 1) * LANES] < LANES, first, second))
    return _cat(outs, 1)


def _pack_cols(flags, r, oc, dg, ea, no, first, second, own_top, to_chip, to_far, strip):
    rows = r.shape[0]
    lane = _iota((1, LANES), 1)
    on_top = flags[0] == 1
    row_even = flags[1] == 0
    col_even = flags[2] == 0

    def store(at, count, west, east):
        to_chip[at : at + count, :] = jnp.where(col_even, east, west)
        to_far[at : at + count, :] = jnp.where(col_even, west, east)

    def packed(pieces):
        west = east = None
        for f, (left, right) in enumerate(pieces):
            a = left if f == 0 else pltpu.roll(left, W * f, 1)
            b = pltpu.roll(right, W * f + W, 1)
            if f == 0:
                west, east = (a, b)
            else:
                here = lane >= W * f
                west = jnp.where(here, a, west)
                east = jnp.where(here, b, east)
        used = lane < 5 * W
        return (jnp.where(used, west, 0.0), jnp.where(used, east, 0.0))

    zero = jnp.zeros((W, LANES), F32)
    for start in range(0, rows, 32):
        span = pl.ds(start, 32)
        west, east = packed(
            [(x[span, :LANES].astype(F32), x[span, LANES:].astype(F32)) for x in (r, oc, dg, ea, no)]
        )
        store(8 + start, 32, west, east)
    for base, blank, choose in ((4, 0, row_even), (8 + rows, 12 + rows, jnp.logical_not(row_even))):
        pieces = []
        for f in range(5):
            x = jnp.where(choose, second[W * f : W * f + W, :], first[W * f : W * f + W, :])
            pieces.append((x[:, :LANES], x[:, LANES:]))
        west, east = packed(pieces)
        store(base, W, west, east)
        store(blank, W, zero, zero)

    @pl.when(on_top)
    def _():
        for f in range(5):
            strip[8 * f : 8 * f + W, :] = own_top[W * f : W * f + W, :]
            strip[8 * f + W : 8 * f + 8, :] = second[W * f : W * f + W, :]
        strip[40:48, :] = jnp.zeros((8, 2 * LANES), F32)
        own_partner, far_partner = (own_top[20:21, :], second[20:21, :])
        strip[40:41, :] = own_partner
        strip[41:42, :] = far_partner
        row = _iota((8, 1), 0)
        index = jnp.where(row < 4, own_partner, far_partner).astype(jnp.int32) & (2 * LANES - 1)
        masked = strip[0:8, :] * strip[8:16, :]
        first = _pick(pltpu.roll(masked, 4, 0), index)
        north = strip[32:40, :]
        coef = 0.5 * (north + _pick(pltpu.roll(north, 4, 0), index))
        strip[35:36, :] = coef[3:4, :]
        strip[39:40, :] = coef[7:8, :]
        strip[42:43, :] = first[3:4, :]
        strip[43:44, :] = first[7:8, :]

    base = rows + 16
    for half in range(2):
        part = strip[:, half * LANES : (half + 1) * LANES]
        to_chip[base + STRIP * half : base + STRIP * (half + 1), :] = part
        to_far[base + STRIP * half : base + STRIP * (half + 1), :] = part


def pack_cols(flags, fields, first, second, own_top):
    rows, cols = fields[0].shape
    message = jax.ShapeDtypeStruct((rows + 16 + 2 * STRIP, LANES), F32)
    vmem = pl.BlockSpec(memory_space=pltpu.VMEM)
    return pl.pallas_call(
        _pack_cols,
        in_specs=[pl.BlockSpec(memory_space=pltpu.SMEM)] + [vmem] * 8,
        out_specs=(vmem,) * 3,
        out_shape=(message, message, jax.ShapeDtypeStruct((STRIP, cols), F32)),
        name="pack_cols",
    )(flags, *fields, first, second, own_top)


def _lanes_left(x):
    return pltpu.roll(x, x.shape[1] - 1, 1)


def _lanes_right(x):
    return pltpu.roll(x, 1, 1)


def _strip_levels(strip, sides, fold):
    row = _iota((8, 1), 0)
    lane = _iota((1, LANES), 1)
    near = row < 4

    def far(side, at, count):
        return _cat([sides[side, at : at + count, :], sides[side, STRIP + at : STRIP + at + count, :]], 1)

    def assembled(mine, east, west, east2, west2):
        left = jnp.where(near, west, east)
        right = jnp.where(near, east, west)
        tail = jnp.where(
            lane < 64,
            jnp.where(near, east2, west2)[:, :LANES],
            jnp.where(near, west2, east2)[:, LANES:],
        )
        return _cat([left, mine, right, tail], 1)

    def field(f):
        s = 8 * f
        return assembled(strip[s : s + 8, :], *(far(side, s, 8) for side in range(4)))

    def pair(at):
        def one(a, b):
            return jnp.where(near, a, b)

        return assembled(
            one(strip[at : at + 1, :], strip[at + 1 : at + 2, :]),
            *(one(far(side, at, 1), far(side, at + 1, 1)) for side in range(4)),
        )

    r, oc, dg, ea, no = [field(f) for f in range(5)]
    index = pair(40).astype(jnp.int32) & (2 * LANES - 1)
    neighbour = pair(42)
    edge = (row & 3) == 3
    fc = jnp.where(edge, no, 0.0)
    no = jnp.where(edge, 0.0, no)
    scale = 2.0 / HALF
    ocs = oc * scale
    ce = ea * ocs * _lanes_left(oc)
    cw = _lanes_right(ce)
    cn = no * ocs * pltpu.roll(oc, 7, 0)
    cs = pltpu.roll(cn, 1, 0)
    cf = fc * ocs
    d = (dg - MID) * scale + ocs * (ea + _lanes_right(ea) + no + pltpu.roll(no, 1, 0) + fc)

    def main_row(x):
        x = x[3:4, :]
        return _cat([x[:, 256:512], jnp.where(lane < 64, x[:, 512:640], x[:, 128:256])], 1)

    fold[4:5, :] = main_row(cf)
    previous = None
    value = r
    for k in range(4):
        term = cf * neighbour
        fold[k : k + 1, :] = main_row(term)
        if k == 3:
            break
        new = (
            d * value
            - ce * _lanes_left(value)
            - cw * _lanes_right(value)
            - cn * pltpu.roll(value, 7, 0)
            - cs * pltpu.roll(value, 1, 0)
            - term
        )
        new = 0.5 * new if k == 0 else new - previous
        previous, value = (value, new)
        swapped = pltpu.roll(value * oc, 4, 0)
        blocks = [swapped[:, 256 * j : 256 * j + 256] for j in range(3)]
        picked = [_pick(blocks[2 - j], index[:, 256 * j : 256 * j + 256]) for j in range(3)]
        neighbour = _cat([*picked, jnp.zeros((8, LANES), F32)], 1)


def _basis(flags, r, oc, dg, ea, no, first, second, chip, far, far2, chip2, strip, t1, t2, t3, t4, moments, ext, coef, fold, sides):
    rows, cols = r.shape
    pad = 16
    high = rows + pad
    wide = cols + LANES
    lane = _iota((1, LANES), 1)
    total = rows + 2 * pad
    on_top = flags[0] == 1
    row_even = flags[1] == 0
    col_even = flags[2] == 0
    for f, own in enumerate((r, oc, dg, ea, no)):
        ext[f, 0 : pad, :cols] = jnp.zeros((pad, cols), F32)
        ext[f, high : high + pad, :cols] = jnp.zeros((pad, cols), F32)
        ext[f, pad:high, :cols] = own[...].astype(F32)
        one, two = (first[W * f : W * f + W, :], second[W * f : W * f + W, :])
        ext[f, pad - W : pad, :cols] = jnp.where(row_even, two, one)
        ext[f, high : high + W, :cols] = jnp.where(row_even, one, two)
        ext[f, 0:8, cols:] = jnp.zeros((8, LANES), F32)
        ext[f, total - 8 : total, cols:] = jnp.zeros((8, LANES), F32)
        east = jnp.where(col_even, chip[0 : rows + 16, :], far[0 : rows + 16, :])
        if f:
            east = pltpu.roll(east, LANES - W * f, 1)
        west = jnp.where(col_even, far[0 : rows + 16, :], chip[0 : rows + 16, :])
        west = pltpu.roll(west, LANES - W - W * f, 1)
        halo = jnp.where(lane < W, east, jnp.where(lane >= LANES - W, west, 0.0))
        ext[f, 8 : 8 + rows + 16, cols:] = halo
    for k in (5, 6, 7):
        ext[k, 0:8, :] = jnp.zeros((8, wide), F32)
        ext[k, total - 8 : total, :] = jnp.zeros((8, wide), F32)

    @pl.when(on_top)
    def _():
        ext[4, high - 1 : high, :] = jnp.zeros((1, wide), F32)
        tail = slice(rows + 16, rows + 16 + 2 * STRIP)
        sides[0] = jnp.where(col_even, chip[tail, :], far[tail, :])
        sides[1] = jnp.where(col_even, far[tail, :], chip[tail, :])
        sides[2] = jnp.where(col_even, chip2[tail, :], far2[tail, :])
        sides[3] = jnp.where(col_even, far2[tail, :], chip2[tail, :])
        _strip_levels(strip, sides, fold)

    @pl.when(jnp.logical_not(on_top))
    def _():
        fold[...] = jnp.zeros_like(fold)

    scale = 2.0 / HALF
    last = (high - 8) // 8
    sub = _iota((8, 1), 0)
    for t in range(1, total // 8 - 1):
        a = 8 * t
        o = ext[1, a : a + 8, :]
        os = o * scale
        e = ext[3, a : a + 8, :]
        n = ext[4, a : a + 8, :]
        d = (ext[2, a : a + 8, :] - MID) * scale + os * (e + _lanes_right(e) + n + ext[4, a - 1 : a + 7, :])
        if t == last:
            d = d + jnp.where(sub == 7, fold[4:5, :], 0.0)
        coef[0, a : a + 8, :] = d
        coef[1, a : a + 8, :] = e * os * _lanes_left(o)
        coef[2, a : a + 8, :] = n * os * ext[1, a + 1 : a + 9, :]
    coef[2, 0:8, :] = jnp.zeros((8, wide), F32)

    outs = (t1, t2, t3, t4)
    sums = []
    own = r[0:8, :]
    square = own * own
    for t in range(1, rows // 8):
        own = r[8 * t : 8 * t + 8, :]
        square = square + own * own
    sums.append(square)
    for k in range(4):
        source = 0 if k == 0 else 4 + k
        square = cross = None
        tiles = range(2, total // 8 - 2) if k == 3 else range(1, total // 8 - 1)
        for t in tiles:
            a = 8 * t
            v = ext[source, a : a + 8, :]
            ce = coef[1, a : a + 8, :]
            new = (
                coef[0, a : a + 8, :] * v
                - ce * _lanes_left(v)
                - _lanes_right(ce * 1.0) * _lanes_right(v)
                - coef[2, a : a + 8, :] * ext[source, a + 1 : a + 9, :]
                - coef[2, a - 1 : a + 7, :] * ext[source, a - 1 : a + 7, :]
            )
            if t == last:
                new = new - jnp.where(sub == 7, fold[k : k + 1, :], 0.0)
            if k == 0:
                new = 0.5 * new
            else:
                new = new - ext[0 if k == 1 else 3 + k, a : a + 8, :]
            if k < 3:
                ext[5 + k, a : a + 8, :] = new
            if pad <= a < high:
                mine = new[:, :cols]
                outs[k][a - pad : a - pad + 8, :] = mine
                x = mine * v[:, :cols]
                cross = x if cross is None else cross + x
                if k < 3:
                    s = mine * mine
                    square = s if square is None else square + s
        sums.append(cross)
        if k < 3:
            sums.append(square)
    out = jnp.zeros((1, LANES), F32)
    for k, x in enumerate(sums):
        folded = x[:, :LANES] + x[:, LANES:]
        one = jnp.sum(jnp.sum(folded, axis=0, keepdims=True), axis=1, keepdims=True)
        out = jnp.where(lane == k, one, out)
    moments[...] = jnp.broadcast_to(out, moments.shape)


def basis(flags, fields, first, second, chip, far, far2, chip2, strip, devices):
    rows, cols = fields[0].shape
    vmem = pl.BlockSpec(memory_space=pltpu.VMEM)
    out = jax.ShapeDtypeStruct((rows, cols), F32)
    return pl.pallas_call(
        _basis,
        in_specs=[pl.BlockSpec(memory_space=pltpu.SMEM)] + [vmem] * 12,
        out_specs=(vmem,) * 5,
        out_shape=(out,) * 4 + (jax.ShapeDtypeStruct((devices, LANES), F32),),
        scratch_shapes=[
            pltpu.VMEM((8, rows + 32, cols + LANES), F32),
            pltpu.VMEM((3, rows + 32, cols + LANES), F32),
            pltpu.VMEM((8, cols + LANES), F32),
            pltpu.VMEM((4, 2 * STRIP, LANES), F32),
        ],
        name="basis",
    )(flags, *fields, first, second, chip, far, far2, chip2, strip)


def _combine(gathered, r, t1, t2, t3, t4, x_out, r_out):
    sums = jnp.sum(gathered[...], axis=0, keepdims=True)
    m = [sums[:, k : k + 1] for k in range(8)]
    nu = [m[0], m[1]]
    for k in range(1, 4):
        nu += [2.0 * m[2 * k] - m[0], 2.0 * m[2 * k + 1] - m[1]]
    gram = {}
    for i in range(4):
        for j in range(i, 5):
            if i == 0:
                gram[i, j] = nu[j]
            else:
                gram[i, j] = 0.5 * (nu[i + j] + nu[j - i])
            gram[j, i] = gram[i, j]

    def dot(a, b):
        total = None
        for i, p in enumerate(a):
            inner = None
            for j, q in enumerate(b):
                term = q * gram[i, j]
                inner = term if inner is None else inner + term
            inner = p * inner
            total = inner if total is None else total + inner
        return total

    def apply(v):
        n = len(v)
        out = [MID * x for x in v] + [None]
        for j, x in enumerate(v):
            if j == 0:
                up = HALF * x
            else:
                up = (0.5 * HALF) * x
                out[j - 1] = out[j - 1] + up
            out[j + 1] = up if out[j + 1] is None else out[j + 1] + up
        return out

    def add(a, s, b):
        out = []
        for i in range(max(len(a), len(b))):
            if i >= len(a):
                out.append(s * b[i])
            elif i >= len(b):
                out.append(a[i])
            else:
                out.append(a[i] + s * b[i])
        return out

    one = jnp.ones((1, 1), F32)
    solution_field, residual, direction = ([], [one], [one])
    norm_now = m[0]
    for iteration in range(ITERS):
        image = apply(direction)
        alpha = norm_now / dot(direction, image)
        solution_field = add(solution_field, alpha, direction)
        residual = add(residual, -alpha, image)
        if iteration + 1 < ITERS:
            norm_next = dot(residual, residual)
            direction = add(residual, norm_next / norm_now, direction)
            norm_now = norm_next
    basis_refs = (r, t1, t2, t3, t4)
    for start in range(0, r.shape[0], 8):
        span = pl.ds(start, 8)
        tiles = [ref[span, :] for ref in basis_refs]
        x = solution_field[0] * tiles[0]
        z = residual[0] * tiles[0]
        for k in range(1, 5):
            if k < 4:
                x = x + solution_field[k] * tiles[k]
            z = z + residual[k] * tiles[k]
        x_out[span, :] = x
        r_out[span, :] = z


def combine(gathered, r, t1, t2, t3, t4):
    vmem = pl.BlockSpec(memory_space=pltpu.VMEM)
    out = jax.ShapeDtypeStruct(r.shape, F32)
    return pl.pallas_call(
        _combine, in_specs=[vmem] * 6, out_specs=(vmem,) * 2, out_shape=(out, out), name="combine"
    )(gathered, r, t1, t2, t3, t4)


def local(right_side, diagonal, east_coef, north_coef, land_sea, fold_partner):
    cols = right_side.shape[1]
    lats, lons = (lax.axis_size(LAT), lax.axis_size(LON))
    devices = lats * lons
    lat, lon = (lax.axis_index(LAT), lax.axis_index(LON))
    flags = jnp.stack([(lat == lats - 1).astype(jnp.int32), lat % 2, lon % 2])
    fields = (right_side, land_sea, diagonal, east_coef, north_coef)

    def swap(x, partner, rows=range(lats)):
        pairs = []
        for i in rows:
            for j in range(lons):
                there = partner(i, j)
                if there is not None:
                    pairs.append((i * lons + j, there[0] * lons + there[1] % lons))
        return lax.ppermute(x, LAT_LON, pairs)

    def second_row(i, j):
        if i == lats - 1:
            return (i, lons - 1 - j)
        if i == 0:
            return None
        return (i + 1 if i % 2 else i - 1, j)

    def off_chip(i, j):
        return (i, j + 1 if j % 2 else j - 1)

    def on_chip(i, j):
        return (i, j ^ 1)

    top = (lats - 1,)
    to_first, to_second = pack_rows(flags, fields, fold_partner.reshape(1, cols))
    first = swap(to_first, lambda i, j: (i ^ 1, j))
    second = swap(to_second, second_row)
    to_chip, to_far, strip = pack_cols(flags, fields, first, second, to_second)
    chip = swap(to_chip, on_chip)
    far = swap(to_far, off_chip)
    far2 = swap(chip, off_chip, top)
    chip2 = swap(far, on_chip, top)
    t1, t2, t3, t4, moments = basis(flags, fields, first, second, chip, far, far2, chip2, strip, devices)
    gathered = lax.all_to_all(moments, LAT_LON, 0, 0)
    return combine(gathered, right_side, t1, t2, t3, t4)


def solution(mesh):
    torus = Mesh(mesh.devices.reshape(2, 4, 2, 4, 2), ("lat_0", "lat_1", "lon_0", "lon_1", "lon_2"))
    placed = (P(LAT, LON), P(LAT, LON), P(LAT, LON), P(LAT, LON), P(LAT, LON), P(LON))
    return jax.shard_map(
        local, mesh=torus, in_specs=placed, out_specs=(P(LAT, LON), P(LAT, LON)), check_vma=False
    )
```

```python
import functools

import jax
import jax.numpy as jnp
from jax import lax
from jax.experimental import pallas as pl
from jax.experimental.pallas import tpu as pltpu
from jax.sharding import Mesh
from jax.sharding import PartitionSpec as P

ITERS = 4
LAT_LON = ("lat_0", "lat_1", "lon_0", "lon_1", "lon_2")
LAT = ("lat_0", "lat_1")
LON = ("lon_0", "lon_1", "lon_2")
MID = 4.6
HALF = 4.4
F32 = jnp.float32
W = 4
LANES = 128
GRANT = 16 << 20
STRIP = 48


def _iota(shape, axis):
    return lax.broadcasted_iota(jnp.int32, shape, axis)


def _cat(parts, axis):
    return jnp.concatenate(parts, axis=axis)


def _pack_rows(*refs):
    fields, partner = (refs[:5], refs[5])
    first, second, floats, ints, order, done = refs[6:]
    rows = fields[0].shape[0]
    even = lax.axis_index(LAT) % 2 == 0
    copies = []
    for f, x in enumerate(fields):
        for h, start in enumerate((0, rows - 8)):
            target = ints.at[h] if f == 1 else floats.at[f, h]
            copies.append(pltpu.make_async_copy(x.at[pl.ds(start, 8), :], target, done.at[2 * f + h]))
    copies.append(pltpu.make_async_copy(partner, order, done.at[10]))
    for copy in copies:
        copy.start()
    for copy in copies:
        copy.wait()
    for f in range(5):
        x = ints if f == 1 else floats.at[f]
        low = x[0, 0:W, :].astype(F32)
        high = x[1, 8 - W : 8, :].astype(F32)
        first[W * f : W * f + W, :] = jnp.where(even, high, low)
        second[W * f : W * f + W, :] = jnp.where(even, low, high)
    first[20:24, :] = jnp.zeros((4, first.shape[1]), F32)
    second[20:24, :] = jnp.broadcast_to(order[...].astype(F32), (4, first.shape[1]))


def pack_rows(fields, partner):
    cols = fields[0].shape[1]
    out = jax.ShapeDtypeStruct((24, cols), F32)
    vmem = pl.BlockSpec(memory_space=pltpu.VMEM)
    return pl.pallas_call(
        _pack_rows,
        in_specs=[pl.BlockSpec(memory_space=pltpu.HBM)] * 6,
        out_specs=(vmem,) * 2,
        out_shape=(out, out),
        scratch_shapes=[
            pltpu.VMEM((5, 2, 8, cols), F32),
            pltpu.VMEM((2, 8, cols), jnp.int32),
            pltpu.VMEM((1, cols), jnp.int32),
            pltpu.SemaphoreType.DMA((11,)),
        ],
        compiler_params=pltpu.CompilerParams(vmem_limit_bytes=GRANT),
        name="pack_rows",
    )(*fields, partner)


def _pick(source, index):
    low = index & (LANES - 1)
    outs = []
    for t in range(2):
        at = low[:, t * LANES : (t + 1) * LANES]
        first = jnp.take_along_axis(source[:, :LANES], at, axis=1)
        second = jnp.take_along_axis(source[:, LANES:], at, axis=1)
        outs.append(jnp.where(index[:, t * LANES : (t + 1) * LANES] < LANES, first, second))
    return _cat(outs, 1)


def _pack_cols(r, oc, dg, ea, no, first, second, own_top, to_chip, to_far, strip):
    rows = r.shape[0]
    lane = _iota((1, LANES), 1)
    on_top = lax.axis_index(LAT) == lax.axis_size(LAT) - 1
    row_even = lax.axis_index(LAT) % 2 == 0
    col_even = lax.axis_index(LON) % 2 == 0

    def store(at, count, west, east):
        to_chip[at : at + count, :] = jnp.where(col_even, east, west)
        to_far[at : at + count, :] = jnp.where(col_even, west, east)

    def packed(pieces):
        west = east = None
        for f, (left, right) in enumerate(pieces):
            a = left if f == 0 else pltpu.roll(left, W * f, 1)
            b = pltpu.roll(right, W * f + W, 1)
            if f == 0:
                west, east = (a, b)
            else:
                here = lane >= W * f
                west = jnp.where(here, a, west)
                east = jnp.where(here, b, east)
        used = lane < 5 * W
        return (jnp.where(used, west, 0.0), jnp.where(used, east, 0.0))

    zero = jnp.zeros((W, LANES), F32)
    for start in range(0, rows, 32):
        span = pl.ds(start, 32)
        west, east = packed(
            [(x[span, :LANES].astype(F32), x[span, LANES:].astype(F32)) for x in (r, oc, dg, ea, no)]
        )
        store(8 + start, 32, west, east)
    for base, blank, choose in ((4, 0, row_even), (8 + rows, 12 + rows, jnp.logical_not(row_even))):
        pieces = []
        for f in range(5):
            x = jnp.where(choose, second[W * f : W * f + W, :], first[W * f : W * f + W, :])
            pieces.append((x[:, :LANES], x[:, LANES:]))
        west, east = packed(pieces)
        store(base, W, west, east)
        store(blank, W, zero, zero)

    @pl.when(on_top)
    def _():
        for f in range(5):
            strip[8 * f : 8 * f + W, :] = own_top[W * f : W * f + W, :]
            strip[8 * f + W : 8 * f + 8, :] = second[W * f : W * f + W, :]
        strip[40:48, :] = jnp.zeros((8, 2 * LANES), F32)
        own_partner, far_partner = (own_top[20:21, :], second[20:21, :])
        strip[40:41, :] = own_partner
        strip[41:42, :] = far_partner
        row = _iota((8, 1), 0)
        index = jnp.where(row < 4, own_partner, far_partner).astype(jnp.int32) & (2 * LANES - 1)
        masked = strip[0:8, :] * strip[8:16, :]
        first = _pick(pltpu.roll(masked, 4, 0), index)
        north = strip[32:40, :]
        coef = 0.5 * (north + _pick(pltpu.roll(north, 4, 0), index))
        strip[35:36, :] = coef[3:4, :]
        strip[39:40, :] = coef[7:8, :]
        strip[42:43, :] = first[3:4, :]
        strip[43:44, :] = first[7:8, :]

    base = rows + 16
    for half in range(2):
        part = strip[:, half * LANES : (half + 1) * LANES]
        to_chip[base + STRIP * half : base + STRIP * (half + 1), :] = part
        to_far[base + STRIP * half : base + STRIP * (half + 1), :] = part


def pack_cols(fields, first, second, own_top):
    rows, cols = fields[0].shape
    message = jax.ShapeDtypeStruct((rows + 16 + 2 * STRIP, LANES), F32)
    vmem = pl.BlockSpec(memory_space=pltpu.VMEM)
    return pl.pallas_call(
        _pack_cols,
        in_specs=[vmem] * 8,
        out_specs=(vmem,) * 3,
        out_shape=(message, message, jax.ShapeDtypeStruct((STRIP, cols), F32)),
        compiler_params=pltpu.CompilerParams(vmem_limit_bytes=GRANT),
        name="pack_cols",
    )(*fields, first, second, own_top)


def _lanes_left(x):
    return pltpu.roll(x, x.shape[1] - 1, 1)


def _lanes_right(x):
    return pltpu.roll(x, 1, 1)


def _strip_levels(strip, sides, fold):
    row = _iota((8, 1), 0)
    lane = _iota((1, LANES), 1)
    near = row < 4

    def far(side, at, count):
        return _cat([sides[side, at : at + count, :], sides[side, STRIP + at : STRIP + at + count, :]], 1)

    def assembled(mine, east, west, east2, west2):
        left = jnp.where(near, west, east)
        right = jnp.where(near, east, west)
        tail = jnp.where(
            lane < 64,
            jnp.where(near, east2, west2)[:, :LANES],
            jnp.where(near, west2, east2)[:, LANES:],
        )
        return _cat([left, mine, right, tail], 1)

    def field(f):
        s = 8 * f
        return assembled(strip[s : s + 8, :], *(far(side, s, 8) for side in range(4)))

    def pair(at):
        def one(a, b):
            return jnp.where(near, a, b)

        return assembled(
            one(strip[at : at + 1, :], strip[at + 1 : at + 2, :]),
            *(one(far(side, at, 1), far(side, at + 1, 1)) for side in range(4)),
        )

    r, oc, dg, ea, no = [field(f) for f in range(5)]
    index = pair(40).astype(jnp.int32) & (2 * LANES - 1)
    neighbour = pair(42)
    edge = (row & 3) == 3
    fc = jnp.where(edge, no, 0.0)
    no = jnp.where(edge, 0.0, no)
    scale = 2.0 / HALF
    ocs = oc * scale
    ce = ea * ocs * _lanes_left(oc)
    cw = _lanes_right(ce)
    cn = no * ocs * pltpu.roll(oc, 7, 0)
    cs = pltpu.roll(cn, 1, 0)
    cf = fc * ocs
    d = (dg - MID) * scale + ocs * (ea + _lanes_right(ea) + no + pltpu.roll(no, 1, 0) + fc)

    def main_row(x):
        x = x[3:4, :]
        return _cat([x[:, 256:512], jnp.where(lane < 64, x[:, 512:640], x[:, 128:256])], 1)

    fold[4:5, :] = main_row(cf)
    previous = None
    value = r
    for k in range(4):
        term = cf * neighbour
        fold[k : k + 1, :] = main_row(term)
        if k == 3:
            break
        new = (
            d * value
            - ce * _lanes_left(value)
            - cw * _lanes_right(value)
            - cn * pltpu.roll(value, 7, 0)
            - cs * pltpu.roll(value, 1, 0)
            - term
        )
        new = 0.5 * new if k == 0 else new - previous
        previous, value = (value, new)
        swapped = pltpu.roll(value * oc, 4, 0)
        blocks = [swapped[:, 256 * j : 256 * j + 256] for j in range(3)]
        picked = [_pick(blocks[2 - j], index[:, 256 * j : 256 * j + 256]) for j in range(3)]
        neighbour = _cat([*picked, jnp.zeros((8, LANES), F32)], 1)


def _basis(r, oc, dg, ea, no, first, second, chip, far, far2, chip2, strip, t1, t2, t3, t4, moments, ext, coef, fold, sides):
    rows, cols = r.shape
    pad = 16
    high = rows + pad
    wide = cols + LANES
    lane = _iota((1, LANES), 1)
    total = rows + 2 * pad
    on_top = lax.axis_index(LAT) == lax.axis_size(LAT) - 1
    row_even = lax.axis_index(LAT) % 2 == 0
    col_even = lax.axis_index(LON) % 2 == 0
    for f, own in enumerate((r, oc, dg, ea, no)):
        ext[f, 0 : pad, :cols] = jnp.zeros((pad, cols), F32)
        ext[f, high : high + pad, :cols] = jnp.zeros((pad, cols), F32)
        ext[f, pad:high, :cols] = own[...].astype(F32)
        one, two = (first[W * f : W * f + W, :], second[W * f : W * f + W, :])
        ext[f, pad - W : pad, :cols] = jnp.where(row_even, two, one)
        ext[f, high : high + W, :cols] = jnp.where(row_even, one, two)
        ext[f, 0:8, cols:] = jnp.zeros((8, LANES), F32)
        ext[f, total - 8 : total, cols:] = jnp.zeros((8, LANES), F32)
        east = jnp.where(col_even, chip[0 : rows + 16, :], far[0 : rows + 16, :])
        if f:
            east = pltpu.roll(east, LANES - W * f, 1)
        west = jnp.where(col_even, far[0 : rows + 16, :], chip[0 : rows + 16, :])
        west = pltpu.roll(west, LANES - W - W * f, 1)
        halo = jnp.where(lane < W, east, jnp.where(lane >= LANES - W, west, 0.0))
        ext[f, 8 : 8 + rows + 16, cols:] = halo
    for k in (5, 6, 7):
        ext[k, 0:8, :] = jnp.zeros((8, wide), F32)
        ext[k, total - 8 : total, :] = jnp.zeros((8, wide), F32)

    @pl.when(on_top)
    def _():
        ext[4, high - 1 : high, :] = jnp.zeros((1, wide), F32)
        tail = slice(rows + 16, rows + 16 + 2 * STRIP)
        sides[0] = jnp.where(col_even, chip[tail, :], far[tail, :])
        sides[1] = jnp.where(col_even, far[tail, :], chip[tail, :])
        sides[2] = jnp.where(col_even, chip2[tail, :], far2[tail, :])
        sides[3] = jnp.where(col_even, far2[tail, :], chip2[tail, :])
        _strip_levels(strip, sides, fold)

    @pl.when(jnp.logical_not(on_top))
    def _():
        fold[...] = jnp.zeros_like(fold)

    scale = 2.0 / HALF
    last = (high - 8) // 8
    sub = _iota((8, 1), 0)
    for t in range(1, total // 8 - 1):
        a = 8 * t
        o = ext[1, a : a + 8, :]
        os = o * scale
        e = ext[3, a : a + 8, :]
        n = ext[4, a : a + 8, :]
        d = (ext[2, a : a + 8, :] - MID) * scale + os * (e + _lanes_right(e) + n + ext[4, a - 1 : a + 7, :])
        if t == last:
            d = d + jnp.where(sub == 7, fold[4:5, :], 0.0)
        coef[0, a : a + 8, :] = d
        coef[1, a : a + 8, :] = e * os * _lanes_left(o)
        coef[2, a : a + 8, :] = n * os * ext[1, a + 1 : a + 9, :]
    coef[2, 0:8, :] = jnp.zeros((8, wide), F32)

    outs = (t1, t2, t3, t4)
    sums = []
    own = r[0:8, :]
    square = own * own
    for t in range(1, rows // 8):
        own = r[8 * t : 8 * t + 8, :]
        square = square + own * own
    sums.append(square)
    for k in range(4):
        source = 0 if k == 0 else 4 + k
        square = cross = None
        tiles = range(2, total // 8 - 2) if k == 3 else range(1, total // 8 - 1)
        for t in tiles:
            a = 8 * t
            v = ext[source, a : a + 8, :]
            ce = coef[1, a : a + 8, :]
            new = (
                coef[0, a : a + 8, :] * v
                - ce * _lanes_left(v)
                - _lanes_right(ce * 1.0) * _lanes_right(v)
                - coef[2, a : a + 8, :] * ext[source, a + 1 : a + 9, :]
                - coef[2, a - 1 : a + 7, :] * ext[source, a - 1 : a + 7, :]
            )
            if t == last:
                new = new - jnp.where(sub == 7, fold[k : k + 1, :], 0.0)
            if k == 0:
                new = 0.5 * new
            else:
                new = new - ext[0 if k == 1 else 3 + k, a : a + 8, :]
            if k < 3:
                ext[5 + k, a : a + 8, :] = new
            if pad <= a < high:
                mine = new[:, :cols]
                outs[k][a - pad : a - pad + 8, :] = mine
                x = mine * v[:, :cols]
                cross = x if cross is None else cross + x
                if k < 3:
                    s = mine * mine
                    square = s if square is None else square + s
        sums.append(cross)
        if k < 3:
            sums.append(square)
    out = jnp.zeros((1, LANES), F32)
    for k, x in enumerate(sums):
        folded = x[:, :LANES] + x[:, LANES:]
        one = jnp.sum(jnp.sum(folded, axis=0, keepdims=True), axis=1, keepdims=True)
        out = jnp.where(lane == k, one, out)
    moments[...] = jnp.broadcast_to(out, moments.shape)


def basis(fields, first, second, chip, far, far2, chip2, strip, devices):
    rows, cols = fields[0].shape
    vmem = pl.BlockSpec(memory_space=pltpu.VMEM)
    out = jax.ShapeDtypeStruct((rows, cols), F32)
    return pl.pallas_call(
        _basis,
        in_specs=[vmem] * 12,
        out_specs=(vmem,) * 5,
        out_shape=(out,) * 4 + (jax.ShapeDtypeStruct((devices, LANES), F32),),
        scratch_shapes=[
            pltpu.VMEM((8, rows + 32, cols + LANES), F32),
            pltpu.VMEM((3, rows + 32, cols + LANES), F32),
            pltpu.VMEM((8, cols + LANES), F32),
            pltpu.VMEM((4, 2 * STRIP, LANES), F32),
        ],
        compiler_params=pltpu.CompilerParams(vmem_limit_bytes=GRANT),
        name="basis",
    )(*fields, first, second, chip, far, far2, chip2, strip)


def _combine(gathered, r, t1, t2, t3, t4, x_out, r_out):
    sums = jnp.sum(gathered[...], axis=0, keepdims=True)
    m = [sums[:, k : k + 1] for k in range(8)]
    nu = [m[0], m[1]]
    for k in range(1, 4):
        nu += [2.0 * m[2 * k] - m[0], 2.0 * m[2 * k + 1] - m[1]]
    gram = {}
    for i in range(4):
        for j in range(i, 5):
            if i == 0:
                gram[i, j] = nu[j]
            else:
                gram[i, j] = 0.5 * (nu[i + j] + nu[j - i])
            gram[j, i] = gram[i, j]

    def dot(a, b):
        total = None
        for i, p in enumerate(a):
            inner = None
            for j, q in enumerate(b):
                term = q * gram[i, j]
                inner = term if inner is None else inner + term
            inner = p * inner
            total = inner if total is None else total + inner
        return total

    def apply(v):
        n = len(v)
        out = [MID * x for x in v] + [None]
        for j, x in enumerate(v):
            if j == 0:
                up = HALF * x
            else:
                up = (0.5 * HALF) * x
                out[j - 1] = out[j - 1] + up
            out[j + 1] = up if out[j + 1] is None else out[j + 1] + up
        return out

    def add(a, s, b):
        out = []
        for i in range(max(len(a), len(b))):
            if i >= len(a):
                out.append(s * b[i])
            elif i >= len(b):
                out.append(a[i])
            else:
                out.append(a[i] + s * b[i])
        return out

    one = jnp.ones((1, 1), F32)
    solution_field, residual, direction = ([], [one], [one])
    norm_now = m[0]
    for iteration in range(ITERS):
        image = apply(direction)
        alpha = norm_now / dot(direction, image)
        solution_field = add(solution_field, alpha, direction)
        residual = add(residual, -alpha, image)
        if iteration + 1 < ITERS:
            norm_next = dot(residual, residual)
            direction = add(residual, norm_next / norm_now, direction)
            norm_now = norm_next
    basis_refs = (r, t1, t2, t3, t4)
    for start in range(0, r.shape[0], 8):
        span = pl.ds(start, 8)
        tiles = [ref[span, :] for ref in basis_refs]
        x = solution_field[0] * tiles[0]
        z = residual[0] * tiles[0]
        for k in range(1, 5):
            if k < 4:
                x = x + solution_field[k] * tiles[k]
            z = z + residual[k] * tiles[k]
        x_out[span, :] = x
        r_out[span, :] = z


def combine(gathered, r, t1, t2, t3, t4):
    vmem = pl.BlockSpec(memory_space=pltpu.VMEM)
    out = jax.ShapeDtypeStruct(r.shape, F32)
    return pl.pallas_call(
        _combine,
        in_specs=[vmem] * 6,
        out_specs=(vmem,) * 2,
        out_shape=(out, out),
        compiler_params=pltpu.CompilerParams(vmem_limit_bytes=GRANT),
        name="combine",
    )(gathered, r, t1, t2, t3, t4)


def local(right_side, diagonal, east_coef, north_coef, land_sea, fold_partner):
    cols = right_side.shape[1]
    lats, lons = (lax.axis_size(LAT), lax.axis_size(LON))
    devices = lats * lons
    fields = (right_side, land_sea, diagonal, east_coef, north_coef)

    def swap(x, partner, rows=range(lats)):
        pairs = []
        for i in rows:
            for j in range(lons):
                there = partner(i, j)
                if there is not None:
                    pairs.append((i * lons + j, there[0] * lons + there[1] % lons))
        return lax.ppermute(x, LAT_LON, pairs)

    def second_row(i, j):
        if i == lats - 1:
            return (i, lons - 1 - j)
        if i == 0:
            return None
        return (i + 1 if i % 2 else i - 1, j)

    def off_chip(i, j):
        return (i, j + 1 if j % 2 else j - 1)

    def on_chip(i, j):
        return (i, j ^ 1)

    top = (lats - 1,)
    kept = [pltpu.with_memory_space_constraint(x, pltpu.HBM) for x in (*fields, fold_partner.reshape(1, cols))]
    to_first, to_second = pack_rows(kept[:5], kept[5])
    first = swap(to_first, lambda i, j: (i ^ 1, j))
    second = swap(to_second, second_row)
    to_chip, to_far, strip = pack_cols(fields, first, second, to_second)
    chip = swap(to_chip, on_chip)
    far = swap(to_far, off_chip)
    far2 = swap(chip, off_chip, top)
    chip2 = swap(far, on_chip, top)
    t1, t2, t3, t4, moments = basis(fields, first, second, chip, far, far2, chip2, strip, devices)
    gathered = lax.all_to_all(moments, LAT_LON, 0, 0)
    return combine(gathered, right_side, t1, t2, t3, t4)


def solution(mesh):
    torus = Mesh(mesh.devices.reshape(2, 4, 2, 4, 2), ("lat_0", "lat_1", "lon_0", "lon_1", "lon_2"))
    placed = (P(LAT, LON), P(LAT, LON), P(LAT, LON), P(LAT, LON), P(LAT, LON), P(LON))
    return jax.shard_map(
        local, mesh=torus, in_specs=placed, out_specs=(P(LAT, LON), P(LAT, LON)), check_vma=False
    )
```

```python
import functools

import jax
import jax.numpy as jnp
from jax import lax
from jax.experimental import pallas as pl
from jax.experimental.pallas import tpu as pltpu
from jax.sharding import Mesh
from jax.sharding import PartitionSpec as P

ITERS = 4
LAT_LON = ("lat_0", "lat_1", "lon_0", "lon_1", "lon_2")
LAT = ("lat_0", "lat_1")
LON = ("lon_0", "lon_1", "lon_2")
MID = 4.6
HALF = 4.4
F32 = jnp.float32
W = 4
LANES = 128
GRANT = 16 << 20
STRIP = 48


def _iota(shape, axis):
    return lax.broadcasted_iota(jnp.int32, shape, axis)


def _cat(parts, axis):
    return jnp.concatenate(parts, axis=axis)


def _pack_rows(*refs):
    fields, partner = (refs[:5], refs[5])
    record, floats, ints, order, done = refs[6:]
    rows = fields[0].shape[0]
    copies = []
    for f, x in enumerate(fields):
        for h, start in enumerate((0, rows - 8)):
            target = ints.at[h] if f == 1 else floats.at[f, h]
            copies.append(pltpu.make_async_copy(x.at[pl.ds(start, 8), :], target, done.at[2 * f + h]))
    copies.append(pltpu.make_async_copy(partner, order, done.at[10]))
    for copy in copies:
        copy.start()
    for copy in copies:
        copy.wait()
    for f in range(5):
        x = ints if f == 1 else floats.at[f]
        record[W * f : W * f + W, :] = x[0, 0:W, :].astype(F32)
        record[24 + W * f : 24 + W * f + W, :] = x[1, 8 - W : 8, :].astype(F32)
    record[20:24, :] = jnp.zeros((4, record.shape[1]), F32)
    record[44:48, :] = jnp.broadcast_to(order[...].astype(F32), (4, record.shape[1]))


def pack_rows(fields, partner):
    cols = fields[0].shape[1]
    return pl.pallas_call(
        _pack_rows,
        in_specs=[pl.BlockSpec(memory_space=pltpu.HBM)] * 6,
        out_specs=pl.BlockSpec(memory_space=pltpu.VMEM),
        out_shape=jax.ShapeDtypeStruct((48, cols), F32),
        scratch_shapes=[
            pltpu.VMEM((5, 2, 8, cols), F32),
            pltpu.VMEM((2, 8, cols), jnp.int32),
            pltpu.VMEM((1, cols), jnp.int32),
            pltpu.SemaphoreType.DMA((11,)),
        ],
        compiler_params=pltpu.CompilerParams(vmem_limit_bytes=GRANT),
        name="pack_rows",
    )(*fields, partner)


def _places():
    lat, core = (lax.axis_index(LAT), lax.axis_index(LON) % 2)
    return (lat == lax.axis_size(LAT) - 1, core == 0, (lat + core) % 2 == 0)


def _pack_chip(mine, sibling, out):
    _, western, northern = _places()
    for slot in range(2):
        first, second = (mine, sibling) if slot == 0 else (sibling, mine)
        low = jnp.where(western, first[0:24, :], second[0:24, :])
        high = jnp.where(western, first[24:48, :], second[24:48, :])
        out[24 * slot : 24 * slot + 24, :] = jnp.where(northern, high, low)


def pack_chip(mine, sibling):
    vmem = pl.BlockSpec(memory_space=pltpu.VMEM)
    return pl.pallas_call(
        _pack_chip,
        in_specs=[vmem] * 2,
        out_specs=vmem,
        out_shape=jax.ShapeDtypeStruct(mine.shape, F32),
        compiler_params=pltpu.CompilerParams(vmem_limit_bytes=GRANT),
        name="pack_chip",
    )(mine, sibling)


def _pick(source, index):
    low = index & (LANES - 1)
    outs = []
    for t in range(2):
        at = low[:, t * LANES : (t + 1) * LANES]
        first = jnp.take_along_axis(source[:, :LANES], at, axis=1)
        second = jnp.take_along_axis(source[:, LANES:], at, axis=1)
        outs.append(jnp.where(index[:, t * LANES : (t + 1) * LANES] < LANES, first, second))
    return _cat(outs, 1)


def _edges(lane, left, right):
    return jnp.where(lane < LANES // 2, left, right)


def _pack_cols(r, oc, dg, ea, no, mine, sibling, traded, told, to_chip, to_far, halo, strips):
    rows = r.shape[0]
    lane = _iota((1, LANES), 1)
    on_top, western, northern = _places()
    slots = []
    for choose in (northern, jnp.logical_not(northern)):
        slots.append([jnp.where(choose, traded[k : k + 24, :], told[k : k + 24, :]) for k in (0, 24)])
    north, south = slots
    halo[0:24, :] = jnp.where(western, north[0], north[1])
    halo[24:48, :] = jnp.where(western, south[0], south[1])

    def store(at, count, west, east):
        to_chip[at : at + count, :] = jnp.where(western, east, west)
        to_far[at : at + count, :] = jnp.where(western, west, east)

    def packed(pieces):
        west = east = None
        for f, (left, right) in enumerate(pieces):
            a = left if f == 0 else pltpu.roll(left, W * f, 1)
            b = pltpu.roll(right, W * f + W, 1)
            if f == 0:
                west, east = (a, b)
            else:
                here = lane >= W * f
                west = jnp.where(here, a, west)
                east = jnp.where(here, b, east)
        used = lane < 5 * W
        return (jnp.where(used, west, 0.0), jnp.where(used, east, 0.0))

    zero = jnp.zeros((W, LANES), F32)
    for start in range(0, rows, 32):
        span = pl.ds(start, 32)
        west, east = packed(
            [(x[span, :LANES].astype(F32), x[span, LANES:].astype(F32)) for x in (r, oc, dg, ea, no)]
        )
        store(8 + start, 32, west, east)
    for base, blank, source in ((4, 0, 24), (8 + rows, 12 + rows, 0)):
        pieces = []
        for f in range(5):
            x = halo[source + W * f : source + W * f + W, :]
            pieces.append((x[:, :LANES], x[:, LANES:]))
        west, east = packed(pieces)
        store(base, W, west, east)
        store(blank, W, zero, zero)

    @pl.when(on_top)
    def _():
        row = _iota((8, 1), 0)
        for s, near, far in (
            (0, mine, jnp.where(western, north[1], north[0])),
            (STRIP, sibling, jnp.where(western, north[0], north[1])),
        ):
            for f in range(5):
                strips[s + 8 * f : s + 8 * f + W, :] = near[24 + W * f : 24 + W * f + W, :]
                strips[s + 8 * f + W : s + 8 * f + 8, :] = far[W * f : W * f + W, :]
            strips[s + 40 : s + 48, :] = jnp.zeros((8, 2 * LANES), F32)
            near_partner, far_partner = (near[44:45, :], far[20:21, :])
            strips[s + 40 : s + 41, :] = near_partner
            strips[s + 41 : s + 42, :] = far_partner
            index = jnp.where(row < 4, near_partner, far_partner).astype(jnp.int32) & (2 * LANES - 1)
            masked = strips[s : s + 8, :] * strips[s + 8 : s + 16, :]
            first = _pick(pltpu.roll(masked, 4, 0), index)
            coef = strips[s + 32 : s + 40, :]
            coef = 0.5 * (coef + _pick(pltpu.roll(coef, 4, 0), index))
            strips[s + 35 : s + 36, :] = coef[3:4, :]
            strips[s + 39 : s + 40, :] = coef[7:8, :]
            strips[s + 42 : s + 43, :] = first[3:4, :]
            strips[s + 43 : s + 44, :] = first[7:8, :]

    base = rows + 16
    to_far[base : base + STRIP, :] = strips[0:STRIP, :LANES]
    to_far[base + STRIP : base + 2 * STRIP, :] = strips[0:STRIP, LANES:]
    to_far[base + 2 * STRIP : base + 3 * STRIP, :] = _edges(
        lane, strips[STRIP : 2 * STRIP, :LANES], strips[STRIP : 2 * STRIP, LANES:]
    )


def pack_cols(fields, mine, sibling, traded, told):
    rows, cols = fields[0].shape

    def out(*shape):
        return jax.ShapeDtypeStruct(shape, F32)

    vmem = pl.BlockSpec(memory_space=pltpu.VMEM)
    return pl.pallas_call(
        _pack_cols,
        in_specs=[vmem] * 9,
        out_specs=(vmem,) * 4,
        out_shape=(
            out(rows + 16, LANES),
            out(rows + 16 + 3 * STRIP, LANES),
            out(48, cols),
            out(2 * STRIP, cols),
        ),
        compiler_params=pltpu.CompilerParams(vmem_limit_bytes=GRANT),
        name="pack_cols",
    )(*fields, mine, sibling, traded, told)


def _lanes_left(x):
    return pltpu.roll(x, x.shape[1] - 1, 1)


def _lanes_right(x):
    return pltpu.roll(x, 1, 1)


def _strip_levels(strips, sides, ends, fold):
    row = _iota((8, 1), 0)
    lane = _iota((1, LANES), 1)
    near = row < 4

    def assembled(mine, east, west, east2, west2):
        left = jnp.where(near, west, east)
        right = jnp.where(near, east, west)
        tail = _edges(lane, jnp.where(near, east2, west2), jnp.where(near, west2, east2))
        return _cat([left, mine, right, tail], 1)

    def field(f):
        s = slice(8 * f, 8 * f + 8)
        return assembled(strips[s, :], sides[0, s, :], sides[1, s, :], ends[0, s, :], ends[1, s, :])

    def pair(at):
        def one(x):
            return jnp.where(near, x[0:1, :], x[1:2, :])

        s = slice(at, at + 2)
        return assembled(
            one(strips[s, :]), one(sides[0, s, :]), one(sides[1, s, :]), one(ends[0, s, :]), one(ends[1, s, :])
        )

    r, oc, dg, ea, no = [field(f) for f in range(5)]
    index = pair(40).astype(jnp.int32) & (2 * LANES - 1)
    neighbour = pair(42)
    edge = (row & 3) == 3
    fc = jnp.where(edge, no, 0.0)
    no = jnp.where(edge, 0.0, no)
    scale = 2.0 / HALF
    ocs = oc * scale
    ce = ea * ocs * _lanes_left(oc)
    cw = _lanes_right(ce)
    cn = no * ocs * pltpu.roll(oc, 7, 0)
    cs = pltpu.roll(cn, 1, 0)
    cf = fc * ocs
    d = (dg - MID) * scale + ocs * (ea + _lanes_right(ea) + no + pltpu.roll(no, 1, 0) + fc)

    def main_row(x):
        x = x[3:4, :]
        return _cat([x[:, 256:512], jnp.where(lane < 64, x[:, 512:640], x[:, 128:256])], 1)

    fold[4:5, :] = main_row(cf)
    previous = None
    value = r
    for k in range(4):
        term = cf * neighbour
        fold[k : k + 1, :] = main_row(term)
        if k == 3:
            break
        new = (
            d * value
            - ce * _lanes_left(value)
            - cw * _lanes_right(value)
            - cn * pltpu.roll(value, 7, 0)
            - cs * pltpu.roll(value, 1, 0)
            - term
        )
        new = 0.5 * new if k == 0 else new - previous
        previous, value = (value, new)
        swapped = pltpu.roll(value * oc, 4, 0)
        blocks = [swapped[:, 256 * j : 256 * j + 256] for j in range(3)]
        picked = [_pick(blocks[2 - j], index[:, 256 * j : 256 * j + 256]) for j in range(3)]
        neighbour = _cat([*picked, jnp.zeros((8, LANES), F32)], 1)


def _basis(r, oc, dg, ea, no, halo, chip, far, chip2, strips, t1, t2, t3, t4, moments, ext, coef, fold, sides, ends):
    rows, cols = r.shape
    pad = 16
    high = rows + pad
    wide = cols + LANES
    lane = _iota((1, LANES), 1)
    total = rows + 2 * pad
    on_top, western, _ = _places()
    for f, own in enumerate((r, oc, dg, ea, no)):
        ext[f, 0 : pad, :cols] = jnp.zeros((pad, cols), F32)
        ext[f, high : high + pad, :cols] = jnp.zeros((pad, cols), F32)
        ext[f, pad:high, :cols] = own[...].astype(F32)
        ext[f, pad - W : pad, :cols] = halo[24 + W * f : 24 + W * f + W, :]
        ext[f, high : high + W, :cols] = halo[W * f : W * f + W, :]
        ext[f, 0:8, cols:] = jnp.zeros((8, LANES), F32)
        ext[f, total - 8 : total, cols:] = jnp.zeros((8, LANES), F32)
        east = jnp.where(western, chip[0 : rows + 16, :], far[0 : rows + 16, :])
        if f:
            east = pltpu.roll(east, LANES - W * f, 1)
        west = jnp.where(western, far[0 : rows + 16, :], chip[0 : rows + 16, :])
        west = pltpu.roll(west, LANES - W - W * f, 1)
        outer = jnp.where(lane < W, east, jnp.where(lane >= LANES - W, west, 0.0))
        ext[f, 8 : 8 + rows + 16, cols:] = outer
    for k in (5, 6, 7):
        ext[k, 0:8, :] = jnp.zeros((8, wide), F32)
        ext[k, total - 8 : total, :] = jnp.zeros((8, wide), F32)

    @pl.when(on_top)
    def _():
        ext[4, high - 1 : high, :] = jnp.zeros((1, wide), F32)
        base = rows + 16
        near = strips[STRIP : 2 * STRIP, :]
        beyond = _cat([far[base : base + STRIP, :], far[base + STRIP : base + 2 * STRIP, :]], 1)
        sides[0] = jnp.where(western, near, beyond)
        sides[1] = jnp.where(western, beyond, near)
        near = _edges(lane, chip2[base : base + STRIP, :], chip2[base + STRIP : base + 2 * STRIP, :])
        beyond = far[base + 2 * STRIP : base + 3 * STRIP, :]
        ends[0] = jnp.where(western, near, beyond)
        ends[1] = jnp.where(western, beyond, near)
        _strip_levels(strips, sides, ends, fold)

    @pl.when(jnp.logical_not(on_top))
    def _():
        fold[...] = jnp.zeros_like(fold)

    scale = 2.0 / HALF
    last = (high - 8) // 8
    sub = _iota((8, 1), 0)
    for t in range(1, total // 8 - 1):
        a = 8 * t
        o = ext[1, a : a + 8, :]
        os = o * scale
        e = ext[3, a : a + 8, :]
        n = ext[4, a : a + 8, :]
        d = (ext[2, a : a + 8, :] - MID) * scale + os * (e + _lanes_right(e) + n + ext[4, a - 1 : a + 7, :])
        if t == last:
            d = d + jnp.where(sub == 7, fold[4:5, :], 0.0)
        coef[0, a : a + 8, :] = d
        coef[1, a : a + 8, :] = e * os * _lanes_left(o)
        coef[2, a : a + 8, :] = n * os * ext[1, a + 1 : a + 9, :]
    coef[2, 0:8, :] = jnp.zeros((8, wide), F32)

    outs = (t1, t2, t3, t4)
    sums = []
    own = r[0:8, :]
    square = own * own
    for t in range(1, rows // 8):
        own = r[8 * t : 8 * t + 8, :]
        square = square + own * own
    sums.append(square)
    for k in range(4):
        source = 0 if k == 0 else 4 + k
        square = cross = None
        tiles = range(2, total // 8 - 2) if k == 3 else range(1, total // 8 - 1)
        for t in tiles:
            a = 8 * t
            v = ext[source, a : a + 8, :]
            ce = coef[1, a : a + 8, :]
            new = (
                coef[0, a : a + 8, :] * v
                - ce * _lanes_left(v)
                - _lanes_right(ce * 1.0) * _lanes_right(v)
                - coef[2, a : a + 8, :] * ext[source, a + 1 : a + 9, :]
                - coef[2, a - 1 : a + 7, :] * ext[source, a - 1 : a + 7, :]
            )
            if t == last:
                new = new - jnp.where(sub == 7, fold[k : k + 1, :], 0.0)
            if k == 0:
                new = 0.5 * new
            else:
                new = new - ext[0 if k == 1 else 3 + k, a : a + 8, :]
            if k < 3:
                ext[5 + k, a : a + 8, :] = new
            if pad <= a < high:
                mine = new[:, :cols]
                outs[k][a - pad : a - pad + 8, :] = mine
                x = mine * v[:, :cols]
                cross = x if cross is None else cross + x
                if k < 3:
                    s = mine * mine
                    square = s if square is None else square + s
        sums.append(cross)
        if k < 3:
            sums.append(square)
    out = jnp.zeros((1, LANES), F32)
    for k, x in enumerate(sums):
        folded = x[:, :LANES] + x[:, LANES:]
        one = jnp.sum(jnp.sum(folded, axis=0, keepdims=True), axis=1, keepdims=True)
        out = jnp.where(lane == k, one, out)
    moments[...] = jnp.broadcast_to(out, moments.shape)


def basis(fields, halo, chip, far, chip2, strips, devices):
    rows, cols = fields[0].shape
    vmem = pl.BlockSpec(memory_space=pltpu.VMEM)
    out = jax.ShapeDtypeStruct((rows, cols), F32)
    return pl.pallas_call(
        _basis,
        in_specs=[vmem] * 10,
        out_specs=(vmem,) * 5,
        out_shape=(out,) * 4 + (jax.ShapeDtypeStruct((devices, LANES), F32),),
        scratch_shapes=[
            pltpu.VMEM((8, rows + 32, cols + LANES), F32),
            pltpu.VMEM((3, rows + 32, cols + LANES), F32),
            pltpu.VMEM((8, cols + LANES), F32),
            pltpu.VMEM((2, STRIP, cols), F32),
            pltpu.VMEM((2, STRIP, LANES), F32),
        ],
        compiler_params=pltpu.CompilerParams(vmem_limit_bytes=GRANT),
        name="basis",
    )(*fields, halo, chip, far, chip2, strips)


def _combine(gathered, r, t1, t2, t3, t4, x_out, r_out):
    sums = jnp.sum(gathered[...], axis=0, keepdims=True)
    m = [sums[:, k : k + 1] for k in range(8)]
    nu = [m[0], m[1]]
    for k in range(1, 4):
        nu += [2.0 * m[2 * k] - m[0], 2.0 * m[2 * k + 1] - m[1]]
    gram = {}
    for i in range(4):
        for j in range(i, 5):
            if i == 0:
                gram[i, j] = nu[j]
            else:
                gram[i, j] = 0.5 * (nu[i + j] + nu[j - i])
            gram[j, i] = gram[i, j]

    def dot(a, b):
        total = None
        for i, p in enumerate(a):
            inner = None
            for j, q in enumerate(b):
                term = q * gram[i, j]
                inner = term if inner is None else inner + term
            inner = p * inner
            total = inner if total is None else total + inner
        return total

    def apply(v):
        n = len(v)
        out = [MID * x for x in v] + [None]
        for j, x in enumerate(v):
            if j == 0:
                up = HALF * x
            else:
                up = (0.5 * HALF) * x
                out[j - 1] = out[j - 1] + up
            out[j + 1] = up if out[j + 1] is None else out[j + 1] + up
        return out

    def add(a, s, b):
        out = []
        for i in range(max(len(a), len(b))):
            if i >= len(a):
                out.append(s * b[i])
            elif i >= len(b):
                out.append(a[i])
            else:
                out.append(a[i] + s * b[i])
        return out

    one = jnp.ones((1, 1), F32)
    solution_field, residual, direction = ([], [one], [one])
    norm_now = m[0]
    for iteration in range(ITERS):
        image = apply(direction)
        alpha = norm_now / dot(direction, image)
        solution_field = add(solution_field, alpha, direction)
        residual = add(residual, -alpha, image)
        if iteration + 1 < ITERS:
            norm_next = dot(residual, residual)
            direction = add(residual, norm_next / norm_now, direction)
            norm_now = norm_next
    basis_refs = (r, t1, t2, t3, t4)
    for start in range(0, r.shape[0], 8):
        span = pl.ds(start, 8)
        tiles = [ref[span, :] for ref in basis_refs]
        x = solution_field[0] * tiles[0]
        z = residual[0] * tiles[0]
        for k in range(1, 5):
            if k < 4:
                x = x + solution_field[k] * tiles[k]
            z = z + residual[k] * tiles[k]
        x_out[span, :] = x
        r_out[span, :] = z


def combine(gathered, r, t1, t2, t3, t4):
    vmem = pl.BlockSpec(memory_space=pltpu.VMEM)
    out = jax.ShapeDtypeStruct(r.shape, F32)
    return pl.pallas_call(
        _combine,
        in_specs=[vmem] * 6,
        out_specs=(vmem,) * 2,
        out_shape=(out, out),
        compiler_params=pltpu.CompilerParams(vmem_limit_bytes=GRANT),
        name="combine",
    )(gathered, r, t1, t2, t3, t4)


def local(right_side, diagonal, east_coef, north_coef, land_sea, fold_partner):
    cols = right_side.shape[1]
    lats, lons = (lax.axis_size(LAT), lax.axis_size(LON))
    devices = lats * lons
    fields = (right_side, land_sea, diagonal, east_coef, north_coef)

    def swap(x, partner, rows=range(lats)):
        pairs = []
        for i in rows:
            for j in range(lons):
                there = partner(i, j)
                if there is not None:
                    pairs.append((i * lons + j, there[0] * lons + there[1] % lons))
        return lax.ppermute(x, LAT_LON, pairs)

    def row_trade(i, j):
        if (i + j) % 2:
            return (i - 1, j) if i else None
        if i < lats - 1:
            return (i + 1, j)
        return (i, lons - j) if j % 2 else None

    def off_chip(i, j):
        return (i, j + 1 if j % 2 else j - 1)

    def on_chip(i, j):
        return (i, j ^ 1)

    top = (lats - 1,)
    kept = [pltpu.with_memory_space_constraint(x, pltpu.HBM) for x in (*fields, fold_partner.reshape(1, cols))]
    mine = pack_rows(kept[:5], kept[5])
    sibling = swap(mine, on_chip)
    traded = swap(pack_chip(mine, sibling), row_trade)
    told = swap(traded, on_chip)
    to_chip, to_far, halo, strips = pack_cols(fields, mine, sibling, traded, told)
    far = swap(to_far, off_chip)
    chip = swap(to_chip, on_chip)
    chip2 = swap(far, on_chip, top)
    t1, t2, t3, t4, moments = basis(fields, halo, chip, far, chip2, strips, devices)
    gathered = lax.all_to_all(moments, LAT_LON, 0, 0)
    return combine(gathered, right_side, t1, t2, t3, t4)


def solution(mesh):
    torus = Mesh(mesh.devices.reshape(2, 4, 2, 4, 2), ("lat_0", "lat_1", "lon_0", "lon_1", "lon_2"))
    placed = (P(LAT, LON), P(LAT, LON), P(LAT, LON), P(LAT, LON), P(LAT, LON), P(LON))
    return jax.shard_map(
        local, mesh=torus, in_specs=placed, out_specs=(P(LAT, LON), P(LAT, LON)), check_vma=False
    )
```

```python
import functools

import jax
import jax.numpy as jnp
from jax import lax
from jax.experimental import pallas as pl
from jax.experimental.pallas import tpu as pltpu
from jax.sharding import Mesh
from jax.sharding import PartitionSpec as P

ITERS = 4
LAT_LON = ("lat_0", "lat_1", "lon_0", "lon_1", "lon_2")
LAT = ("lat_0", "lat_1")
LON = ("lon_0", "lon_1", "lon_2")
MID = 4.3
HALF = 4.1
LIMIT = 12.0
F32 = jnp.float32
W = 4
LANES = 128
GRANT = 16 << 20
STRIP = 48


def _iota(shape, axis):
    return lax.broadcasted_iota(jnp.int32, shape, axis)


def _cat(parts, axis):
    return jnp.concatenate(parts, axis=axis)


def _pack_rows(*refs):
    fields, partner = (refs[:5], refs[5])
    first, second, floats, ints, order, done = refs[6:]
    rows = fields[0].shape[0]
    even = lax.axis_index(LAT) % 2 == 0
    copies = []
    for f, x in enumerate(fields):
        for h, start in enumerate((0, rows - 8)):
            target = ints.at[h] if f == 1 else floats.at[f, h]
            copies.append(pltpu.make_async_copy(x.at[pl.ds(start, 8), :], target, done.at[2 * f + h]))
    copies.append(pltpu.make_async_copy(partner, order, done.at[10]))
    for copy in copies:
        copy.start()
    for copy in copies:
        copy.wait()
    for f in range(5):
        x = ints if f == 1 else floats.at[f]
        low = x[0, 0:W, :].astype(F32)
        high = x[1, 8 - W : 8, :].astype(F32)
        first[W * f : W * f + W, :] = jnp.where(even, high, low)
        second[W * f : W * f + W, :] = jnp.where(even, low, high)
    first[20:24, :] = jnp.zeros((4, first.shape[1]), F32)
    second[20:24, :] = jnp.broadcast_to(order[...].astype(F32), (4, first.shape[1]))


def pack_rows(fields, partner):
    cols = fields[0].shape[1]
    out = jax.ShapeDtypeStruct((24, cols), F32)
    vmem = pl.BlockSpec(memory_space=pltpu.VMEM)
    return pl.pallas_call(
        _pack_rows,
        in_specs=[pl.BlockSpec(memory_space=pltpu.HBM)] * 6,
        out_specs=(vmem,) * 2,
        out_shape=(out, out),
        scratch_shapes=[
            pltpu.VMEM((5, 2, 8, cols), F32),
            pltpu.VMEM((2, 8, cols), jnp.int32),
            pltpu.VMEM((1, cols), jnp.int32),
            pltpu.SemaphoreType.DMA((11,)),
        ],
        compiler_params=pltpu.CompilerParams(vmem_limit_bytes=GRANT),
        name="pack_rows",
    )(*fields, partner)


def _pick(source, index):
    low = index & (LANES - 1)
    outs = []
    for t in range(2):
        at = low[:, t * LANES : (t + 1) * LANES]
        first = jnp.take_along_axis(source[:, :LANES], at, axis=1)
        second = jnp.take_along_axis(source[:, LANES:], at, axis=1)
        outs.append(jnp.where(index[:, t * LANES : (t + 1) * LANES] < LANES, first, second))
    return _cat(outs, 1)


def _pack_cols(r, oc, dg, ea, no, first, second, own_top, to_chip, to_far, strip):
    rows = r.shape[0]
    lane = _iota((1, LANES), 1)
    on_top = lax.axis_index(LAT) == lax.axis_size(LAT) - 1
    row_even = lax.axis_index(LAT) % 2 == 0
    col_even = lax.axis_index(LON) % 2 == 0

    def store(at, count, west, east):
        to_chip[at : at + count, :] = jnp.where(col_even, east, west)
        to_far[at : at + count, :] = jnp.where(col_even, west, east)

    def packed(pieces):
        west = east = None
        for f, (left, right) in enumerate(pieces):
            a = left if f == 0 else pltpu.roll(left, W * f, 1)
            b = pltpu.roll(right, W * f + W, 1)
            if f == 0:
                west, east = (a, b)
            else:
                here = lane >= W * f
                west = jnp.where(here, a, west)
                east = jnp.where(here, b, east)
        used = lane < 5 * W
        return (jnp.where(used, west, 0.0), jnp.where(used, east, 0.0))

    zero = jnp.zeros((W, LANES), F32)
    for start in range(0, rows, 32):
        span = pl.ds(start, 32)
        west, east = packed(
            [(x[span, :LANES].astype(F32), x[span, LANES:].astype(F32)) for x in (r, oc, dg, ea, no)]
        )
        store(8 + start, 32, west, east)
    for base, blank, choose in ((4, 0, row_even), (8 + rows, 12 + rows, jnp.logical_not(row_even))):
        pieces = []
        for f in range(5):
            x = jnp.where(choose, second[W * f : W * f + W, :], first[W * f : W * f + W, :])
            pieces.append((x[:, :LANES], x[:, LANES:]))
        west, east = packed(pieces)
        store(base, W, west, east)
        store(blank, W, zero, zero)

    @pl.when(on_top)
    def _():
        for f in range(5):
            strip[8 * f : 8 * f + W, :] = own_top[W * f : W * f + W, :]
            strip[8 * f + W : 8 * f + 8, :] = second[W * f : W * f + W, :]
        strip[40:48, :] = jnp.zeros((8, 2 * LANES), F32)
        own_partner, far_partner = (own_top[20:21, :], second[20:21, :])
        strip[40:41, :] = own_partner
        strip[41:42, :] = far_partner
        row = _iota((8, 1), 0)
        index = jnp.where(row < 4, own_partner, far_partner).astype(jnp.int32) & (2 * LANES - 1)
        masked = strip[0:8, :] * strip[8:16, :]
        first = _pick(pltpu.roll(masked, 4, 0), index)
        north = strip[32:40, :]
        coef = 0.5 * (north + _pick(pltpu.roll(north, 4, 0), index))
        strip[35:36, :] = coef[3:4, :]
        strip[39:40, :] = coef[7:8, :]
        strip[42:43, :] = first[3:4, :]
        strip[43:44, :] = first[7:8, :]

    base = rows + 16
    for half in range(2):
        part = strip[:, half * LANES : (half + 1) * LANES]
        to_chip[base + STRIP * half : base + STRIP * (half + 1), :] = part
        to_far[base + STRIP * half : base + STRIP * (half + 1), :] = part


def pack_cols(fields, first, second, own_top):
    rows, cols = fields[0].shape
    message = jax.ShapeDtypeStruct((rows + 16 + 2 * STRIP, LANES), F32)
    vmem = pl.BlockSpec(memory_space=pltpu.VMEM)
    return pl.pallas_call(
        _pack_cols,
        in_specs=[vmem] * 8,
        out_specs=(vmem,) * 3,
        out_shape=(message, message, jax.ShapeDtypeStruct((STRIP, cols), F32)),
        compiler_params=pltpu.CompilerParams(vmem_limit_bytes=GRANT),
        name="pack_cols",
    )(*fields, first, second, own_top)


def _lanes_left(x):
    return pltpu.roll(x, x.shape[1] - 1, 1)


def _lanes_right(x):
    return pltpu.roll(x, 1, 1)


def _strip_levels(strip, sides, fold):
    row = _iota((8, 1), 0)
    lane = _iota((1, LANES), 1)
    near = row < 4

    def far(side, at, count):
        return _cat([sides[side, at : at + count, :], sides[side, STRIP + at : STRIP + at + count, :]], 1)

    def assembled(mine, east, west, east2, west2):
        left = jnp.where(near, west, east)
        right = jnp.where(near, east, west)
        tail = jnp.where(
            lane < 64,
            jnp.where(near, east2, west2)[:, :LANES],
            jnp.where(near, west2, east2)[:, LANES:],
        )
        return _cat([left, mine, right, tail], 1)

    def field(f):
        s = 8 * f
        return assembled(strip[s : s + 8, :], *(far(side, s, 8) for side in range(4)))

    def pair(at):
        def one(a, b):
            return jnp.where(near, a, b)

        return assembled(
            one(strip[at : at + 1, :], strip[at + 1 : at + 2, :]),
            *(one(far(side, at, 1), far(side, at + 1, 1)) for side in range(4)),
        )

    r, oc, dg, ea, no = [field(f) for f in range(5)]
    index = pair(40).astype(jnp.int32) & (2 * LANES - 1)
    neighbour = pair(42)
    edge = (row & 3) == 3
    fc = jnp.where(edge, no, 0.0)
    no = jnp.where(edge, 0.0, no)
    scale = 2.0 / HALF
    ocs = oc * scale
    ce = ea * ocs * _lanes_left(oc)
    cw = _lanes_right(ce)
    cn = no * ocs * pltpu.roll(oc, 7, 0)
    cs = pltpu.roll(cn, 1, 0)
    cf = fc * ocs
    d = (dg - MID) * scale + ocs * (ea + _lanes_right(ea) + no + pltpu.roll(no, 1, 0) + fc)

    def main_row(x):
        x = x[3:4, :]
        return _cat([x[:, 256:512], jnp.where(lane < 64, x[:, 512:640], x[:, 128:256])], 1)

    fold[4:5, :] = main_row(cf)
    previous = None
    value = r
    for k in range(4):
        term = cf * neighbour
        fold[k : k + 1, :] = main_row(term)
        if k == 3:
            break
        new = (
            d * value
            - ce * _lanes_left(value)
            - cw * _lanes_right(value)
            - cn * pltpu.roll(value, 7, 0)
            - cs * pltpu.roll(value, 1, 0)
            - term
        )
        new = 0.5 * new if k == 0 else new - previous
        previous, value = (value, new)
        swapped = pltpu.roll(value * oc, 4, 0)
        blocks = [swapped[:, 256 * j : 256 * j + 256] for j in range(3)]
        picked = [_pick(blocks[2 - j], index[:, 256 * j : 256 * j + 256]) for j in range(3)]
        neighbour = _cat([*picked, jnp.zeros((8, LANES), F32)], 1)


def _basis(r, oc, dg, ea, no, first, second, chip, far, far2, chip2, strip, t1, t2, t3, t4, moments, ext, coef, fold, sides):
    rows, cols = r.shape
    pad = 16
    high = rows + pad
    wide = cols + LANES
    lane = _iota((1, LANES), 1)
    total = rows + 2 * pad
    on_top = lax.axis_index(LAT) == lax.axis_size(LAT) - 1
    row_even = lax.axis_index(LAT) % 2 == 0
    col_even = lax.axis_index(LON) % 2 == 0
    for f, own in enumerate((r, oc, dg, ea, no)):
        ext[f, 0 : pad, :cols] = jnp.zeros((pad, cols), F32)
        ext[f, high : high + pad, :cols] = jnp.zeros((pad, cols), F32)
        ext[f, pad:high, :cols] = own[...].astype(F32)
        one, two = (first[W * f : W * f + W, :], second[W * f : W * f + W, :])
        ext[f, pad - W : pad, :cols] = jnp.where(row_even, two, one)
        ext[f, high : high + W, :cols] = jnp.where(row_even, one, two)
        ext[f, 0:8, cols:] = jnp.zeros((8, LANES), F32)
        ext[f, total - 8 : total, cols:] = jnp.zeros((8, LANES), F32)
        east = jnp.where(col_even, chip[0 : rows + 16, :], far[0 : rows + 16, :])
        if f:
            east = pltpu.roll(east, LANES - W * f, 1)
        west = jnp.where(col_even, far[0 : rows + 16, :], chip[0 : rows + 16, :])
        west = pltpu.roll(west, LANES - W - W * f, 1)
        halo = jnp.where(lane < W, east, jnp.where(lane >= LANES - W, west, 0.0))
        ext[f, 8 : 8 + rows + 16, cols:] = halo
    for k in (5, 6, 7):
        ext[k, 0:8, :] = jnp.zeros((8, wide), F32)
        ext[k, total - 8 : total, :] = jnp.zeros((8, wide), F32)

    @pl.when(on_top)
    def _():
        ext[4, high - 1 : high, :] = jnp.zeros((1, wide), F32)
        tail = slice(rows + 16, rows + 16 + 2 * STRIP)
        sides[0] = jnp.where(col_even, chip[tail, :], far[tail, :])
        sides[1] = jnp.where(col_even, far[tail, :], chip[tail, :])
        sides[2] = jnp.where(col_even, chip2[tail, :], far2[tail, :])
        sides[3] = jnp.where(col_even, far2[tail, :], chip2[tail, :])
        _strip_levels(strip, sides, fold)

    @pl.when(jnp.logical_not(on_top))
    def _():
        fold[...] = jnp.zeros_like(fold)

    scale = 2.0 / HALF
    last = (high - 8) // 8
    sub = _iota((8, 1), 0)
    for t in range(1, total // 8 - 1):
        a = 8 * t
        o = ext[1, a : a + 8, :]
        os = o * scale
        e = ext[3, a : a + 8, :]
        n = ext[4, a : a + 8, :]
        d = (ext[2, a : a + 8, :] - MID) * scale + os * (e + _lanes_right(e) + n + ext[4, a - 1 : a + 7, :])
        if t == last:
            d = d + jnp.where(sub == 7, fold[4:5, :], 0.0)
        coef[0, a : a + 8, :] = d
        coef[1, a : a + 8, :] = e * os * _lanes_left(o)
        coef[2, a : a + 8, :] = n * os * ext[1, a + 1 : a + 9, :]
    coef[2, 0:8, :] = jnp.zeros((8, wide), F32)

    outs = (t1, t2, t3, t4)
    sums = []
    own = r[0:8, :]
    square = own * own
    for t in range(1, rows // 8):
        own = r[8 * t : 8 * t + 8, :]
        square = square + own * own
    sums.append(square)
    for k in range(4):
        source = 0 if k == 0 else 4 + k
        square = cross = None
        tiles = range(2, total // 8 - 2) if k == 3 else range(1, total // 8 - 1)
        for t in tiles:
            a = 8 * t
            v = ext[source, a : a + 8, :]
            ce = coef[1, a : a + 8, :]
            new = (
                coef[0, a : a + 8, :] * v
                - ce * _lanes_left(v)
                - _lanes_right(ce * 1.0) * _lanes_right(v)
                - coef[2, a : a + 8, :] * ext[source, a + 1 : a + 9, :]
                - coef[2, a - 1 : a + 7, :] * ext[source, a - 1 : a + 7, :]
            )
            if t == last:
                new = new - jnp.where(sub == 7, fold[k : k + 1, :], 0.0)
            if k == 0:
                new = 0.5 * new
            else:
                new = new - ext[0 if k == 1 else 3 + k, a : a + 8, :]
            if k < 3:
                ext[5 + k, a : a + 8, :] = new
            if pad <= a < high:
                mine = new[:, :cols]
                outs[k][a - pad : a - pad + 8, :] = mine
                x = mine * v[:, :cols]
                cross = x if cross is None else cross + x
                s = mine * mine
                square = s if square is None else square + s
        sums += [cross, square]
    out = jnp.zeros((1, LANES), F32)
    for k, x in enumerate(sums):
        folded = x[:, :LANES] + x[:, LANES:]
        one = jnp.sum(jnp.sum(folded, axis=0, keepdims=True), axis=1, keepdims=True)
        out = jnp.where(lane == k, one, out)
    moments[...] = jnp.broadcast_to(out, moments.shape)


def basis(fields, first, second, chip, far, far2, chip2, strip, devices):
    rows, cols = fields[0].shape
    vmem = pl.BlockSpec(memory_space=pltpu.VMEM)
    out = jax.ShapeDtypeStruct((rows, cols), F32)
    return pl.pallas_call(
        _basis,
        in_specs=[vmem] * 12,
        out_specs=(vmem,) * 5,
        out_shape=(out,) * 4 + (jax.ShapeDtypeStruct((devices, LANES), F32),),
        scratch_shapes=[
            pltpu.VMEM((8, rows + 32, cols + LANES), F32),
            pltpu.VMEM((3, rows + 32, cols + LANES), F32),
            pltpu.VMEM((8, cols + LANES), F32),
            pltpu.VMEM((4, 2 * STRIP, LANES), F32),
        ],
        compiler_params=pltpu.CompilerParams(vmem_limit_bytes=GRANT),
        name="basis",
    )(*fields, first, second, chip, far, far2, chip2, strip)


def _combine(gathered, r, t1, t2, t3, t4, x_out, r_out, weak):
    sums = jnp.sum(gathered[...], axis=0, keepdims=True)
    m = [sums[:, k : k + 1] for k in range(9)]
    nu = [m[0], m[1]]
    for k in range(1, 4):
        nu += [2.0 * m[2 * k] - m[0], 2.0 * m[2 * k + 1] - m[1]]
    nu.append(2.0 * m[8] - m[0])
    gram = {}
    for i in range(5):
        for j in range(i, 5):
            if i == 0:
                gram[i, j] = nu[j]
            else:
                gram[i, j] = 0.5 * (nu[i + j] + nu[j - i])
            gram[j, i] = gram[i, j]

    def dot(a, b):
        total = None
        for i, p in enumerate(a):
            inner = None
            for j, q in enumerate(b):
                term = q * gram[i, j]
                inner = term if inner is None else inner + term
            inner = p * inner
            total = inner if total is None else total + inner
        return total

    def apply(v):
        n = len(v)
        out = [MID * x for x in v] + [None]
        for j, x in enumerate(v):
            if j == 0:
                up = HALF * x
            else:
                up = (0.5 * HALF) * x
                out[j - 1] = out[j - 1] + up
            out[j + 1] = up if out[j + 1] is None else out[j + 1] + up
        return out

    def add(a, s, b):
        out = []
        for i in range(max(len(a), len(b))):
            if i >= len(a):
                out.append(s * b[i])
            elif i >= len(b):
                out.append(a[i])
            else:
                out.append(a[i] + s * b[i])
        return out

    one = jnp.ones((1, 1), F32)
    solution_field, residual, direction = ([], [one], [one])
    norm_now = m[0]
    for iteration in range(ITERS):
        image = apply(direction)
        alpha = norm_now / dot(direction, image)
        solution_field = add(solution_field, alpha, direction)
        residual = add(residual, -alpha, image)
        if iteration + 1 < ITERS:
            norm_next = dot(residual, residual)
            direction = add(residual, norm_next / norm_now, direction)
            norm_now = norm_next
    size = dot(residual, residual)
    largest = functools.reduce(jnp.maximum, (residual[k] * residual[k] * m[2 * k] for k in range(5)))
    good = largest <= (LIMIT * LIMIT) * size
    weak[0, 0] = 1 - jnp.max(good.astype(jnp.int32))
    basis_refs = (r, t1, t2, t3, t4)
    for start in range(0, r.shape[0], 8):
        span = pl.ds(start, 8)
        tiles = [ref[span, :] for ref in basis_refs]
        x = solution_field[0] * tiles[0]
        z = residual[0] * tiles[0]
        for k in range(1, 5):
            if k < 4:
                x = x + solution_field[k] * tiles[k]
            z = z + residual[k] * tiles[k]
        x_out[span, :] = x
        r_out[span, :] = z


def combine(gathered, r, t1, t2, t3, t4):
    vmem = pl.BlockSpec(memory_space=pltpu.VMEM)
    out = jax.ShapeDtypeStruct(r.shape, F32)
    return pl.pallas_call(
        _combine,
        in_specs=[vmem] * 6,
        out_specs=(vmem, vmem, pl.BlockSpec(memory_space=pltpu.SMEM)),
        out_shape=(out, out, jax.ShapeDtypeStruct((1, 1), jnp.int32)),
        compiler_params=pltpu.CompilerParams(vmem_limit_bytes=GRANT),
        name="combine",
    )(gathered, r, t1, t2, t3, t4)


def shifted(x, axes, dim, up):
    count, length = (lax.axis_size(axes), x.shape[dim])
    ring = [(i, (i + 1) % count) if up else ((i + 1) % count, i) for i in range(count)]
    edge = lax.slice_in_dim(x, length - 1, length, axis=dim) if up else lax.slice_in_dim(x, 0, 1, axis=dim)
    edge = lax.ppermute(edge, axes, ring)
    if up:
        return _cat([edge, lax.slice_in_dim(x, 0, length - 1, axis=dim)], dim)
    return _cat([lax.slice_in_dim(x, 1, length, axis=dim), edge], dim)


def classic(right_side, diagonal, east_coef, north_coef, land_sea, fold_partner):
    row_count, col_count = right_side.shape
    ocean = land_sea.astype(F32)
    on_top = lax.axis_index(LAT) == lax.axis_size(LAT) - 1
    top_row = on_top & (_iota((row_count, 1), 0) == row_count - 1)
    north_inner = jnp.where(top_row, 0.0, north_coef)
    west_coef = shifted(east_coef, LON, 1, True)
    south_coef = shifted(north_inner, LAT, 0, True)
    lons = lax.axis_size(LON)
    columns = fold_partner.astype(jnp.int32) - (lons - 1 - lax.axis_index(LON)) * col_count

    def mirrored(row):
        row = lax.ppermute(row, LON, [(j, lons - 1 - j) for j in range(lons)])
        return jnp.take(row, columns, axis=0)

    top_coef = north_coef[row_count - 1]
    fold_coef = 0.5 * (top_coef + mirrored(top_coef))

    def operate(surface):
        masked = ocean * surface
        spread = east_coef * (masked - shifted(masked, LON, 1, False))
        spread = spread + west_coef * (masked - shifted(masked, LON, 1, True))
        spread = spread + north_inner * (masked - shifted(masked, LAT, 0, False))
        spread = spread + south_coef * (masked - shifted(masked, LAT, 0, True))
        last = masked[row_count - 1]
        fold = fold_coef * (last - mirrored(last))
        spread = spread + jnp.where(top_row, fold[None, :], 0.0)
        return diagonal * surface + ocean * spread

    def total(x):
        return functools.reduce(lax.psum, LAT_LON, jnp.sum(x))

    def step(_, state):
        solution_field, residual, direction, norm_now = state
        image = operate(direction)
        alpha = norm_now / total(direction * image)
        solution_field = solution_field + alpha * direction
        residual = residual - alpha * image
        norm_next = total(residual * residual)
        direction = residual + (norm_next / norm_now) * direction
        return (solution_field, residual, direction, norm_next)

    state = (jnp.zeros_like(right_side), right_side, right_side, total(right_side * right_side))
    return lax.fori_loop(0, ITERS, step, state)[:2]


def local(right_side, diagonal, east_coef, north_coef, land_sea, fold_partner):
    cols = right_side.shape[1]
    lats, lons = (lax.axis_size(LAT), lax.axis_size(LON))
    devices = lats * lons
    fields = (right_side, land_sea, diagonal, east_coef, north_coef)

    def swap(x, partner, rows=range(lats)):
        pairs = []
        for i in rows:
            for j in range(lons):
                there = partner(i, j)
                if there is not None:
                    pairs.append((i * lons + j, there[0] * lons + there[1] % lons))
        return lax.ppermute(x, LAT_LON, pairs)

    def second_row(i, j):
        if i == lats - 1:
            return (i, lons - 1 - j)
        if i == 0:
            return None
        return (i + 1 if i % 2 else i - 1, j)

    def off_chip(i, j):
        return (i, j + 1 if j % 2 else j - 1)

    def on_chip(i, j):
        return (i, j ^ 1)

    top = (lats - 1,)
    kept = [pltpu.with_memory_space_constraint(x, pltpu.HBM) for x in (*fields, fold_partner.reshape(1, cols))]
    to_first, to_second = pack_rows(kept[:5], kept[5])
    first = swap(to_first, lambda i, j: (i ^ 1, j))
    second = swap(to_second, second_row)
    to_chip, to_far, strip = pack_cols(fields, first, second, to_second)
    chip = swap(to_chip, on_chip)
    far = swap(to_far, off_chip)
    far2 = swap(chip, off_chip, top)
    chip2 = swap(far, on_chip, top)
    t1, t2, t3, t4, moments = basis(fields, first, second, chip, far, far2, chip2, strip, devices)
    gathered = lax.all_to_all(moments, LAT_LON, 0, 0)
    solution_field, residual, weak = combine(gathered, right_side, t1, t2, t3, t4)

    def again(state):
        return (jnp.int32(0), *classic(right_side, diagonal, east_coef, north_coef, land_sea, to_second[20]))

    state = (weak[0, 0], solution_field, residual)
    return lax.while_loop(lambda state: state[0] > 0, again, state)[1:]


def solution(mesh):
    torus = Mesh(mesh.devices.reshape(2, 4, 2, 4, 2), ("lat_0", "lat_1", "lon_0", "lon_1", "lon_2"))
    placed = (P(LAT, LON), P(LAT, LON), P(LAT, LON), P(LAT, LON), P(LAT, LON), P(LON))
    return jax.shard_map(
        local, mesh=torus, in_specs=placed, out_specs=(P(LAT, LON), P(LAT, LON)), check_vma=False
    )
```
